32 devices in a mesh: dp: 2 (over x), etp: 4 (over z), ep: 4 (over y, core).
Axes of the slice: x: 2, y: 2, z: 4, core: 2. Of those that a mesh axis runs over, the one named last changes fastest.
Arguments:
- x_in: bfloat16 [1024, 1536], P(('dp', 'ep')), parts along dimension 0
- y_grad: bfloat16 [1024, 1536], P(('dp', 'ep')), parts along dimension 0
- prim_exp: int32 [1024], P(('dp', 'ep')), parts along dimension 0
- alt_exp: int32 [1024], P(('dp', 'ep')), parts along dimension 0
- w_router: bfloat16 [1536, 40], replicated
- exp_gate: bfloat16 [40, 1536, 512], P('ep', None, 'etp')
- exp_up: bfloat16 [40, 1536, 512], P('ep', None, 'etp')
- exp_down: bfloat16 [40, 512, 1536], P('ep', 'etp')
- sh_gate: bfloat16 [1536, 512], P(None, 'etp')
- sh_up: bfloat16 [1536, 512], P(None, 'etp')
- sh_down: bfloat16 [512, 1536], P('etp')
Outputs:
- output 1: bfloat16 [1024, 1536], P(('dp', 'ep')), parts along dimension 0
- output 2: bfloat16 [1024, 1536], P(('dp', 'ep')), parts along dimension 0
- output 3: float32 [80, 1536, 512], P(('dp', 'ep'), None, 'etp'), parts along dimension 0
- output 4: float32 [80, 1536, 512], P(('dp', 'ep'), None, 'etp'), parts along dimension 0
- output 5: float32 [80, 512, 1536], P(('dp', 'ep'), 'etp'), parts along dimension 0
- output 6: float32 [3072, 512], P('dp', 'etp'), parts along dimension 0
- output 7: float32 [3072, 512], P('dp', 'etp'), parts along dimension 0
- output 8: float32 [1024, 1536], P(('dp', 'etp')), parts along dimension 0
- output 9: float32 [3072, 40], P('dp'), parts along dimension 0
There are 2 independent parts. The reference program is written for one: setup_inputs(seed, part) draws one part's arguments, and reference() takes and returns one part's arrays. A program takes and returns all parts, laid end to end along the dimension named above; an argument that names none is the same for every part.
All inputs are finite; a program needn't handle non-finite values.
Results may differ from the reference program's by a relative error of at most 0.00232.
Values are sent between devices in bfloat16 or wider.
A program may use at most 1 GiB of HBM per device.

```python
import jax
import jax.numpy as jnp
from jax import lax

D = 1536
FF = 512
EXPERTS = 40
TOKENS = 512
CAP = 16
EPS = 1e-5


def draw_routes(route_key):
    key_hot, key_pick, key_coin, key_flat, key_alt = jax.random.split(route_key, 5)
    hot_ids = jax.random.permutation(key_hot, EXPERTS)[:3]
    hot_pick = jax.random.randint(key_pick, (TOKENS,), 0, 3)
    hot_coin = jax.random.randint(key_coin, (TOKENS,), 0, 4)
    flat_ids = jax.random.randint(key_flat, (TOKENS,), 0, EXPERTS)
    prim_exp = jnp.where(hot_coin == 0, hot_ids[hot_pick], flat_ids).astype(jnp.int32)
    alt_shift = jax.random.randint(key_alt, (TOKENS,), 1, EXPERTS)
    alt_exp = ((prim_exp + alt_shift) % EXPERTS).astype(jnp.int32)
    return prim_exp, alt_exp


def normal_mat(rand_key, arr_shape, mult_scale):
    return (jax.random.normal(rand_key, arr_shape, jnp.float32) * mult_scale).astype(jnp.bfloat16)


def setup_inputs(seed: int = 0, part: int = 0) -> dict:
    base_key = jax.random.key(seed)
    part_keys = jax.random.split(jax.random.fold_in(base_key, part), 3)
    weight_keys = jax.random.split(base_key, 7)
    prim_exp, alt_exp = draw_routes(part_keys[2])
    return dict(
        x_in=normal_mat(part_keys[0], (TOKENS, D), 1.0),
        y_grad=normal_mat(part_keys[1], (TOKENS, D), 1.0),
        prim_exp=prim_exp,
        alt_exp=alt_exp,
        w_router=normal_mat(weight_keys[0], (D, EXPERTS), D ** -0.5),
        exp_gate=normal_mat(weight_keys[1], (EXPERTS, D, FF), D ** -0.5),
        exp_up=normal_mat(weight_keys[2], (EXPERTS, D, FF), D ** -0.5),
        exp_down=normal_mat(weight_keys[3], (EXPERTS, FF, D), 0.5 * EXPERTS * FF ** -0.5),
        sh_gate=normal_mat(weight_keys[4], (D, FF), D ** -0.5),
        sh_up=normal_mat(weight_keys[5], (D, FF), D ** -0.5),
        sh_down=normal_mat(weight_keys[6], (FF, D), FF ** -0.5),
    )


def exclusive_rank(onehot):
    return jnp.sum((jnp.cumsum(onehot, axis=0) - onehot) * onehot, axis=1)


def route_tokens(prim_exp, alt_exp):
    expert_ids = jnp.arange(EXPERTS)
    one_prim = (prim_exp[:, None] == expert_ids[None, :]).astype(jnp.int32)
    rank_prim = exclusive_rank(one_prim)
    keep_prim = rank_prim < CAP
    kept_count = jnp.minimum(jnp.sum(one_prim, axis=0), CAP)
    overflow = jnp.logical_not(keep_prim).astype(jnp.int32)
    one_alt = (alt_exp[:, None] == expert_ids[None, :]).astype(jnp.int32) * overflow[:, None]
    slot_alt = exclusive_rank(one_alt) + jnp.sum(one_alt * kept_count[None, :], axis=1)
    keep_alt = (overflow == 1) & (slot_alt < CAP)
    assign = jnp.where(keep_prim, prim_exp, jnp.where(keep_alt, alt_exp, -1))
    slot_idx = jnp.where(keep_prim, rank_prim, slot_alt)
    return assign, slot_idx


def glu_forward(tok_rows, w_gate, w_up):
    act_gate = jnp.dot(tok_rows, w_gate, preferred_element_type=jnp.float32)
    act_up = jnp.dot(tok_rows, w_up, preferred_element_type=jnp.float32)
    hidden = (jax.nn.silu(act_gate) * act_up).astype(jnp.bfloat16)
    return hidden, act_gate, act_up


def glu_backward(d_hidden, act_gate, act_up):
    sig_gate = jax.nn.sigmoid(act_gate)
    d_gate = (d_hidden * act_up * sig_gate * (1.0 + act_gate * (1.0 - sig_gate))).astype(jnp.bfloat16)
    d_up = (d_hidden * act_gate * sig_gate).astype(jnp.bfloat16)
    return d_gate, d_up


def expert_forward(packed):
    tok_rows, w_gate, w_up, w_down = packed
    hidden, act_gate, act_up = glu_forward(tok_rows, w_gate, w_up)
    out_rows = jnp.dot(hidden, w_down, preferred_element_type=jnp.float32).astype(jnp.bfloat16)
    return hidden, act_gate, act_up, out_rows


def expert_backward(packed):
    tok_rows, d_rows, hidden, act_gate, act_up, w_gate, w_up, w_down = packed
    d_hidden = jnp.dot(d_rows, w_down.T, preferred_element_type=jnp.float32)
    g_down = jnp.dot(hidden.T, d_rows, preferred_element_type=jnp.float32)
    d_gate, d_up = glu_backward(d_hidden, act_gate, act_up)
    g_gate = jnp.dot(tok_rows.T, d_gate, preferred_element_type=jnp.float32)
    g_up = jnp.dot(tok_rows.T, d_up, preferred_element_type=jnp.float32)
    d_rows_in = (jnp.dot(d_gate, w_gate.T, preferred_element_type=jnp.float32) + jnp.dot(d_up, w_up.T, preferred_element_type=jnp.float32)).astype(jnp.bfloat16)
    return g_gate, g_up, g_down, d_rows_in


def reference(x_in, y_grad, prim_exp, alt_exp, w_router, exp_gate, exp_up, exp_down, sh_gate, sh_up, sh_down):
    x_wide = x_in.astype(jnp.float32)
    inv_rms = lax.rsqrt(jnp.mean(x_wide * x_wide, axis=1, keepdims=True) + EPS)
    normed = (x_wide * inv_rms).astype(jnp.bfloat16)
    gate_probs = jax.nn.softmax(jnp.dot(normed, w_router, preferred_element_type=jnp.float32), axis=1)
    assign, slot_idx = route_tokens(prim_exp, alt_exp)
    flat_pos = jnp.where(assign >= 0, assign * CAP + slot_idx, EXPERTS * CAP)
    slot_table = jnp.full((EXPERTS * CAP + 1,), TOKENS, jnp.int32).at[flat_pos].set(jnp.arange(TOKENS, dtype=jnp.int32))[: EXPERTS * CAP]
    expert_rows = jnp.take(normed, slot_table, axis=0, mode="fill", fill_value=0).reshape(EXPERTS, CAP, D)
    hidden, act_gate, act_up, out_rows = lax.map(expert_forward, (expert_rows, exp_gate, exp_up, exp_down))
    tok_out = jnp.take(out_rows.reshape(EXPERTS * CAP, D), flat_pos, axis=0, mode="fill", fill_value=0).astype(jnp.float32)
    one_assign = (assign[:, None] == jnp.arange(EXPERTS)[None, :]).astype(jnp.float32)
    gate_val = jnp.sum(gate_probs * one_assign, axis=1, keepdims=True)
    sh_hidden, sh_act_gate, sh_act_up = glu_forward(normed, sh_gate, sh_up)
    sh_out = jnp.dot(sh_hidden, sh_down, preferred_element_type=jnp.float32)
    y_out = (x_wide + sh_out + gate_val * tok_out).astype(jnp.bfloat16)
    dy_wide = y_grad.astype(jnp.float32)
    d_route = (gate_val * dy_wide).astype(jnp.bfloat16)
    d_gate_val = jnp.sum(dy_wide * tok_out, axis=1, keepdims=True)
    d_logits = (d_gate_val * gate_val * (one_assign - gate_probs)).astype(jnp.bfloat16)
    g_router = jnp.dot(normed.T, d_logits, preferred_element_type=jnp.float32)
    dn_router = jnp.dot(d_logits, w_router.T, preferred_element_type=jnp.float32)
    sh_d_hidden = jnp.dot(y_grad, sh_down.T, preferred_element_type=jnp.float32)
    g_sh_down = jnp.dot(sh_hidden.T, y_grad, preferred_element_type=jnp.float32)
    sh_d_gate, sh_d_up = glu_backward(sh_d_hidden, sh_act_gate, sh_act_up)
    g_sh_gate = jnp.dot(normed.T, sh_d_gate, preferred_element_type=jnp.float32)
    g_sh_up = jnp.dot(normed.T, sh_d_up, preferred_element_type=jnp.float32)
    dn_shared = jnp.dot(sh_d_gate, sh_gate.T, preferred_element_type=jnp.float32) + jnp.dot(sh_d_up, sh_up.T, preferred_element_type=jnp.float32)
    d_rows = jnp.take(d_route, slot_table, axis=0, mode="fill", fill_value=0).reshape(EXPERTS, CAP, D)
    g_exp_gate, g_exp_up, g_exp_down, d_rows_in = lax.map(expert_backward, (expert_rows, d_rows, hidden, act_gate, act_up, exp_gate, exp_up, exp_down))
    dn_routed = jnp.take(d_rows_in.reshape(EXPERTS * CAP, D), flat_pos, axis=0, mode="fill", fill_value=0).astype(jnp.float32)
    d_normed = dn_shared + dn_router + dn_routed
    norm_proj = jnp.mean(d_normed * x_wide, axis=1, keepdims=True)
    x_grad = (dy_wide + inv_rms * d_normed - x_wide * inv_rms ** 3 * norm_proj).astype(jnp.bfloat16)
    return (y_out, x_grad, g_exp_gate, g_exp_up, g_exp_down, g_sh_gate, g_sh_up, g_sh_down, g_router)
```

```python
import functools

import jax
import jax.numpy as jnp
from jax import lax
from jax.experimental import pallas as pl
from jax.experimental.pallas import tpu as pltpu
from jax.sharding import PartitionSpec as P

EPS = 1e-5
F32 = jnp.float32
BF16 = jnp.bfloat16
MESH = pl.DeviceIdType.MESH
TL = 128
NEP = 4
T = TL * NEP
D = 1536
HD = D // 2
E = 40
EL = 10
CAP = 16
W = 128
NM = 18
MR = 32
NC = 4
CR = TL // NC


def dot(a, b):
    return jnp.dot(a, b, preferred_element_type=F32)


def dot_t(a, b):
    return lax.dot_general(a, b, (((1,), (1,)), ((), ())), preferred_element_type=F32)


def tdot(a, b):
    return lax.dot_general(a, b, (((0,), (0,)), ((), ())), preferred_element_type=F32)


def glu(a, b):
    return (a * jax.nn.sigmoid(a) * b).astype(BF16)


def glu_grads(dh, a, b):
    sig = jax.nn.sigmoid(a)
    d_gate = (dh * b * sig * (1.0 + a * (1.0 - sig))).astype(BF16)
    d_up = (dh * a * sig).astype(BF16)
    return d_gate, d_up


def line_kernel(
    x_h, dy_h, prim_v, alt_v, wr_v, wg_h, wu_h, wd_h, sg_h, su_h, sd_h,
    y_o, dx_o, n_o, dyo_o, nr_o, ur_o, act_o, sact_o, dl_o,
    x_a, dy_a, n_a, u_a, ids, wg, wu, wd, sg, su, sd, nr, ur, act, sact, dl,
    part, recv, o_all, dn_all, yb, dgb, pjb, tgt_v, g_v, df_v, dnr_v,
    xl, wl, sl, ids_s, ids_r, xs, xr, zs, zr, es, er, ys, yr, dgs, dgr, pjs, pjr, outs,
):
    z = lax.axis_index("etp")
    e = lax.axis_index("ep")
    e_y, e_c, e_d = e ^ 2, e ^ 1, e ^ 3
    peers = (e_y, e_c, e_d)
    is_end = (z == 0) | (z == 3)
    is_mid = (z == 1) | (z == 2)
    hs = z // 3

    def rows(j):
        return pl.ds(pl.multiple_of(j * TL, TL), TL)

    mine = rows(e)
    lx = pltpu.make_async_copy(x_h, x_a.at[mine], xl.at[0])
    ldy = pltpu.make_async_copy(dy_h, dy_a.at[mine], xl.at[1])
    lx.start()
    ldy.start()
    shared_loads = [pltpu.make_async_copy(a, b, sl.at[k]) for k, (a, b) in enumerate(((sg_h, sg), (su_h, su), (sd_h, sd)))]
    for c in shared_loads:
        c.start()

    def wload(k, i):
        src, dst = ((wg_h, wg), (wu_h, wu), (wd_h, wd))[k]
        return pltpu.make_async_copy(src.at[i], dst.at[i], wl.at[k, i])

    ids[e] = jnp.zeros((8, TL), F32)
    ids[e, 0:1, :] = prim_v[...].astype(F32)
    ids[e, 1:2, :] = alt_v[...].astype(F32)

    barrier = pltpu.get_barrier_semaphore()
    for q in peers:
        pl.semaphore_signal(barrier, inc=1, device_id={"ep": q}, device_id_type=MESH)
    for k in range(1, 4):
        pl.semaphore_signal(barrier, inc=1, device_id={"etp": lax.rem(z + k, 4)}, device_id_type=MESH)
    pl.semaphore_wait(barrier, 6)

    def rcopy(src, dst, s, r, dev):
        return pltpu.make_async_remote_copy(src_ref=src, dst_ref=dst, send_sem=s, recv_sem=r, device_id=dev, device_id_type=MESH)

    ids_c = [rcopy(ids.at[e], ids.at[e], ids_s.at[k], ids_r.at[k], {"ep": peers[k]}) for k in range(3)]
    for c in ids_c:
        c.start()
    lx.wait()
    x_c, relays = [], []
    for k, buf in enumerate((x_a, dy_a)):
        if k == 1:
            ldy.wait()
        pair = [
            rcopy(buf.at[mine], buf.at[mine], xs.at[k, 0], xr.at[k, 0], {"ep": e_y}),
            rcopy(buf.at[mine], buf.at[mine], xs.at[k, 1], xr.at[k, 1], {"ep": e_c}),
        ]
        for c in pair:
            c.start()
        x_c.append(pair)
        relays.append(rcopy(buf.at[rows(e_y)], buf.at[rows(e_y)], xs.at[k, 2], xr.at[k, 2], {"ep": e_c}))

    def load_body(i, _):
        for k in range(3):
            wload(k, i).start()
        return 0

    lax.fori_loop(0, EL, load_body, 0)

    def line_copy(d, m):
        return rcopy(part.at[d, m], recv.at[d, m], zs.at[d, m], zr.at[d, m], {"etp": jnp.clip(z - 1 + 2 * d, 0, 3)})

    def source_send(m):
        @pl.when(z == 3)
        def _():
            line_copy(0, m).start()

        @pl.when(z == 0)
        def _():
            line_copy(1, m).start()

    def take(d, m):
        line_copy(d, m).wait_recv()
        part[d, m] = part[d, m] + recv[d, m]

    def forward(hop, m):
        @pl.when(is_mid)
        def _():
            d = (2 - z) if hop == 1 else (z - 1)
            take(d, m)
            line_copy(d, m).start()

    def norm(xw):
        inv = lax.rsqrt(jnp.mean(xw * xw, axis=1, keepdims=True) + EPS)
        return inv, (xw * inv).astype(BF16)

    for c in shared_loads:
        c.wait()

    def shared_acts(n, dy):
        a = dot(n, sg[...])
        b = dot(n, su[...])
        h = glu(a, b)
        dg_, du_ = glu_grads(dot_t(dy, sd[...]), a, b)
        return h, dg_, du_

    _, n_own = norm(x_a[mine, :].astype(F32))
    h_s, da_s, db_s = shared_acts(n_own, dy_a[mine, :])
    s_part = dot(h_s, sd[...])
    for k in range(4):
        part[0, k] = s_part[k * MR : (k + 1) * MR, :HD]
        part[1, k] = s_part[k * MR : (k + 1) * MR, HD:]
    dns_part = dot_t(da_s, sg[...]) + dot_t(db_s, su[...])
    for k in range(4):
        part[0, 4 + k] = dns_part[k * MR : (k + 1) * MR, :HD]
        part[1, 4 + k] = dns_part[k * MR : (k + 1) * MR, HD:]
    for m in range(8):
        source_send(m)

    forward(1, 0)

    for c in ids_c:
        c.wait_recv()
    x_c[0][0].wait_recv()
    relays[0].start()
    x_c[0][1].wait_recv()
    relays[0].wait_recv()

    def norm_body(j, _):
        _, n = norm(x_a[rows(j), :].astype(F32))
        n_a[rows(j), :] = n
        return 0

    lax.fori_loop(0, NEP, norm_body, 0)
    forward(1, 1)

    logits = dot(n_a[...], wr_v[...])
    ex = jnp.exp(logits - jnp.max(logits, axis=1, keepdims=True))
    probs = ex / jnp.sum(ex, axis=1, keepdims=True)
    cols = []
    for j in range(NEP):
        block = jnp.concatenate([ids[j], jnp.zeros((TL - 8, TL), F32)], axis=0)
        cols.append(jnp.transpose(block)[:, 0:2])
    idc = jnp.concatenate(cols, axis=0)
    prim, alt = idc[:, 0:1], idc[:, 1:2]
    iota_e = lax.broadcasted_iota(jnp.int32, (T, E), 1).astype(F32)
    one_p = jnp.where(prim == iota_e, 1.0, 0.0)
    earlier = jnp.where(
        lax.broadcasted_iota(jnp.int32, (T, T), 0) > lax.broadcasted_iota(jnp.int32, (T, T), 1), 1.0, 0.0
    ).astype(BF16)
    rank = jnp.sum(dot(earlier, one_p.astype(BF16)) * one_p, axis=1, keepdims=True)
    over = jnp.where(rank < CAP, 0.0, 1.0)
    kept = jnp.minimum(jnp.sum(one_p, axis=0, keepdims=True), float(CAP))
    one_a = jnp.where(alt == iota_e, 1.0, 0.0) * over
    slot_a = jnp.sum((dot(earlier, one_a.astype(BF16)) + kept) * one_a, axis=1, keepdims=True)
    keep_a = over * jnp.where(slot_a < CAP, 1.0, 0.0)
    one_s = one_p * (1.0 - over) + one_a * keep_a
    slot = (1.0 - over) * rank + keep_a * slot_a
    eid = jnp.sum(one_s * iota_e, axis=1, keepdims=True)
    has = (1.0 - over) + keep_a
    tgt_v[...] = jnp.where(has > 0.5, eid * CAP + slot, -1.0)
    g_v[...] = jnp.sum(probs * one_s, axis=1, keepdims=True)
    df_v[...] = one_s - probs

    base = (e * (EL * CAP)).astype(F32)
    pick = jnp.where(
        tgt_v[...] - base == lax.broadcasted_iota(jnp.int32, (T, EL * CAP), 1).astype(F32), 1.0, 0.0
    ).astype(BF16)
    nr[...] = tdot(pick, n_a[...]).astype(BF16)
    forward(1, 2)
    forward(2, 0)
    forward(1, 3)
    forward(2, 1)

    x_c[1][0].wait_recv()
    relays[1].start()
    x_c[1][1].wait_recv()
    relays[1].wait_recv()

    def u_body(j, _):
        u_a[rows(j), :] = (g_v[rows(j), :] * dy_a[rows(j), :].astype(F32)).astype(BF16)
        return 0

    lax.fori_loop(0, NEP, u_body, 0)
    forward(1, 4)
    forward(2, 2)
    ur[...] = tdot(pick, u_a[...]).astype(BF16)

    def pair_body(k, _):
        for half in range(2):
            i = 2 * k + half
            for w in range(3):
                wload(w, i).wait()
            sl16 = pl.ds(pl.multiple_of(i * CAP, CAP), CAP)
            n_i, u_i = nr[sl16, :], ur[sl16, :]
            a = dot(n_i, wg[i])
            b = dot(n_i, wu[i])
            h = glu(a, b)
            da, db = glu_grads(dot_t(u_i, wd[i]), a, b)
            act[0, sl16, :] = h
            act[1, sl16, :] = da
            act[2, sl16, :] = db
            o = dot(h, wd[i])
            r16 = slice(half * CAP, (half + 1) * CAP)
            part[0, 8 + k, r16, :] = o[:, :HD]
            part[1, 8 + k, r16, :] = o[:, HD:]
            dn = dot_t(da, wg[i]) + dot_t(db, wu[i])
            part[0, 13 + k, r16, :] = dn[:, :HD]
            part[1, 13 + k, r16, :] = dn[:, HD:]
        source_send(8 + k)

        @pl.when(k < 3)
        def _():
            forward(1, 5 + k)

        forward(2, 3 + k)
        return 0

    lax.fori_loop(0, EL // 2, pair_body, 0)
    for m in range(13, 18):
        source_send(m)

    stores = [
        pltpu.make_async_copy(n_a, n_o, outs.at[0]),
        pltpu.make_async_copy(dy_a, dyo_o, outs.at[1]),
        pltpu.make_async_copy(nr, nr_o, outs.at[2]),
        pltpu.make_async_copy(ur, ur_o, outs.at[3]),
        pltpu.make_async_copy(act, act_o, outs.at[4]),
    ]
    for c in stores:
        c.start()

    def fwd_body(m, _):
        forward(1, m)
        forward(2, m)
        return 0

    lax.fori_loop(8, NM, fwd_body, 0)

    def sact_body(j, _):
        h, da, db = shared_acts(n_a[rows(j), :], dy_a[rows(j), :])
        sact[0, rows(j), :] = h
        sact[1, rows(j), :] = da
        sact[2, rows(j), :] = db
        return 0

    lax.fori_loop(0, NEP, sact_body, 0)
    st = pltpu.make_async_copy(sact, sact_o, outs.at[5])
    st.start()
    stores.append(st)

    def exchange(t, k, p):
        buf = (o_all, dn_all)[t]
        return rcopy(buf.at[e, k], buf.at[e, k], es.at[t, k, p], er.at[t, k, p], {"ep": peers[p]})

    lanes = pl.ds(pl.multiple_of(hs * HD, 128), HD)

    def place(n_rows, start):
        t_col = tgt_v[pl.ds(start, n_rows), :]
        return jnp.where(
            t_col == lax.broadcasted_iota(jnp.int32, (n_rows, E * CAP), 1).astype(F32), 1.0, 0.0
        ).astype(BF16)

    def col_to_row(col):
        return jnp.transpose(jnp.broadcast_to(col, (TL, TL)))[0:1, :]

    def dg_copy(h, k):
        return rcopy(dgb.at[h], dgb.at[h], dgs.at[k], dgr.at[h], {"etp": lax.rem(z + k + 1, 4)})

    def pj_copy():
        return rcopy(pjb.at[hs], pjb.at[hs], pjs.at[0], pjr.at[0], {"etp": 3 - z})

    def end_take(m, _):
        take(hs, m)
        return 0

    def end_take_o(k, _):
        take(hs, 8 + k)
        o_all[e, k] = part[hs, 8 + k].astype(BF16)
        for p in range(3):
            exchange(0, k, p).start()
        return 0

    def end_take_dn(k, _):
        take(hs, 13 + k)
        dn_all[e, k] = part[hs, 13 + k].astype(BF16)
        for p in range(3):
            exchange(1, k, p).start()
        return 0

    def wait_exchange(t):
        def body(k, _):
            for p in range(3):
                exchange(t, k, p).wait_recv()
            return 0

        lax.fori_loop(0, EL // 2, body, 0)

    def relay_copy(t, h, c):
        return rcopy(yb.at[t, h, c], yb.at[t, h, c], ys.at[t, h, c], yr.at[t, h, c], {"etp": jnp.clip(z + 1 - 2 * h, 0, 3)})

    def relay_start(t):
        for c in range(NC):
            relay_copy(t, hs, c).start()

    @pl.when(is_end)
    def _():
        lax.fori_loop(0, 8, end_take, 0)
        lax.fori_loop(0, EL // 2, end_take_o, 0)
        wait_exchange(0)
        o_flat = o_all[...].reshape(E * CAP, HD)
        for j in range(NEP):
            tok = dot(place(TL, j * TL), o_flat)
            prod = dy_a[j * TL : (j + 1) * TL, lanes].astype(F32) * tok
            dgb[hs, 0:1, j * TL : (j + 1) * TL] = col_to_row(jnp.sum(prod, axis=1, keepdims=True))
        for k in range(3):
            dg_copy(hs, k).start()
        tok = dot(place(TL, pl.multiple_of(e * TL, TL)), o_flat)
        s_own = part[hs, 0:4].reshape(TL, HD)
        y = (x_a[mine, lanes].astype(F32) + s_own + g_v[mine, :] * tok).astype(BF16)
        for c in range(NC):
            yb[0, hs, c] = y[c * CR : (c + 1) * CR, :]
        relay_start(0)

    @pl.when(z != 0)
    def _():
        dg_copy(0, 0).wait_recv()

    @pl.when(z != 3)
    def _():
        dg_copy(1, 0).wait_recv()

    for j in range(NEP):
        row = dgb[0, 0:1, j * TL : (j + 1) * TL] + dgb[1, 0:1, j * TL : (j + 1) * TL]
        dg_col = jnp.transpose(jnp.broadcast_to(row, (TL, TL)))[:, 0:1]
        sl_j = slice(j * TL, (j + 1) * TL)
        dl[sl_j, :] = (dg_col * g_v[sl_j, :] * df_v[sl_j, :]).astype(BF16)
    st = pltpu.make_async_copy(dl, dl_o, outs.at[6])
    st.start()
    stores.append(st)

    def relay_through(t):
        for c in range(NC):
            for h in range(2):
                @pl.when(z != 3 * h)
                def _(h=h, c=c):
                    relay_copy(t, h, c).wait_recv()

                @pl.when(is_mid)
                def _(h=h, c=c):
                    relay_copy(t, h, c).start()

    @pl.when(is_mid)
    def _():
        relay_through(0)

    @pl.when(is_end)
    def _():
        dn_r = dot_t(dl[mine, :], wr_v[...])
        dnr_v[0] = dn_r[:, :HD]
        dnr_v[1] = dn_r[:, HD:]
        lax.fori_loop(0, EL // 2, end_take_dn, 0)
        wait_exchange(1)
        tok = dot(place(TL, pl.multiple_of(e * TL, TL)), dn_all[...].reshape(E * CAP, HD))
        dn = part[hs, 4:8].reshape(TL, HD) + dnr_v[hs] + tok
        dnr_v[hs] = dn
        xh = x_a[mine, lanes].astype(F32)
        pjb[hs, 0:1, :] = col_to_row(jnp.sum(dn * xh, axis=1, keepdims=True))
        pj_copy().start()
        inv, _ = norm(x_a[mine, :].astype(F32))
        pj_copy().wait_recv()
        row = pjb[0, 0:1, :] + pjb[1, 0:1, :]
        proj = jnp.transpose(jnp.broadcast_to(row, (TL, TL)))[:, 0:1] * (1.0 / D)
        dx = (dy_a[mine, lanes].astype(F32) + inv * dnr_v[hs] - x_a[mine, lanes].astype(F32) * (inv * inv * inv) * proj).astype(BF16)
        for c in range(NC):
            yb[1, hs, c] = dx[c * CR : (c + 1) * CR, :]
        relay_start(1)

    @pl.when(is_end)
    def _():
        relay_through(0)

    def out_copies(t, out):
        cs = []
        for h in range(2):
            for c in range(NC):
                cs.append(pltpu.make_async_copy(yb.at[t, h, c], out.at[pl.ds(c * CR, CR), pl.ds(h * HD, HD)], outs.at[7 + t * 2 * NC + h * NC + c]))
        return cs

    oc = out_copies(0, y_o)
    for c in oc:
        c.start()
    stores += oc
    relay_through(1)
    oc = out_copies(1, dx_o)
    for c in oc:
        c.start()
    stores += oc

    for c in ids_c:
        c.wait_send()
    for k in range(2):
        for c in x_c[k]:
            c.wait_send()
        relays[k].wait_send()

    def line_drain(m, _):
        @pl.when(z != 0)
        def _():
            line_copy(0, m).wait_send()

        @pl.when(z != 3)
        def _():
            line_copy(1, m).wait_send()

        return 0

    lax.fori_loop(0, NM, line_drain, 0)

    @pl.when(is_end)
    def _():
        def drain(k, _):
            for t in range(2):
                for p in range(3):
                    exchange(t, k, p).wait_send()
            return 0

        lax.fori_loop(0, EL // 2, drain, 0)
        for k in range(3):
            dg_copy(hs, k).wait_send()
        pj_copy().wait_send()

    for t in range(2):
        for c in range(NC):
            @pl.when(z != 3)
            def _(t=t, c=c):
                relay_copy(t, 0, c).wait_send()

            @pl.when(z != 0)
            def _(t=t, c=c):
                relay_copy(t, 1, c).wait_send()

    for c in stores:
        c.wait()


def grads_kernel(nr, ur, act, gg, gu, gd):
    n, u = nr[...], ur[...]
    gg[0] = tdot(n, act[1])
    gu[0] = tdot(n, act[2])
    gd[0] = tdot(act[0], u)


def solution(mesh):
    tok = P(("dp", "ep"), None)
    ids = P(("dp", "ep"))
    in_specs = (tok, tok, ids, ids, P(None, None), P("ep", None, "etp"), P("ep", None, "etp"), P("ep", "etp", None), P(None, "etp"), P(None, "etp"), P("etp", None))
    out_specs = (tok, tok, P(("dp", "ep"), None, "etp"), P(("dp", "ep"), None, "etp"), P(("dp", "ep"), "etp", None), P("dp", "etp"), P("dp", "etp"), P(("dp", "etp"), None), P("dp", None))
    any_ = pl.BlockSpec(memory_space=pl.ANY)
    vmem = pl.BlockSpec(memory_space=pltpu.VMEM)
    dma = pltpu.SemaphoreType.DMA

    def sds(shape, dtype):
        return jax.ShapeDtypeStruct(shape, dtype)

    def step(x, dy, prim, alt, wr, eg, eu, ed, sg, su, sd):
        outs = [
            sds((TL, D), BF16), sds((TL, D), BF16), sds((T, D), BF16), sds((T, D), BF16),
            sds((EL * CAP, D), BF16), sds((EL * CAP, D), BF16), sds((3, EL * CAP, W), BF16), sds((3, T, W), BF16), sds((T, E), BF16),
        ]
        V = pltpu.VMEM
        scratch = [
            V((T, D), BF16), V((T, D), BF16), V((T, D), BF16), V((T, D), BF16), V((NEP, 8, TL), F32),
            V((EL, D, W), BF16), V((EL, D, W), BF16), V((EL, W, D), BF16), V((D, W), BF16), V((D, W), BF16), V((W, D), BF16),
            V((EL * CAP, D), BF16), V((EL * CAP, D), BF16), V((3, EL * CAP, W), BF16), V((3, T, W), BF16), V((T, E), BF16),
            V((2, NM, MR, HD), F32), V((2, NM, MR, HD), F32), V((NEP, EL // 2, MR, HD), BF16), V((NEP, EL // 2, MR, HD), BF16),
            V((2, 2, NC, CR, HD), BF16), V((2, 8, T), F32), V((2, 8, TL), F32), V((T, 1), F32), V((T, 1), F32), V((T, E), F32), V((2, TL, HD), F32),
            dma((2,)), dma((3, EL)), dma((3,)), dma((3,)), dma((3,)), dma((2, 3)), dma((2, 3)), dma((2, NM)), dma((2, NM)),
            dma((2, EL // 2, 3)), dma((2, EL // 2, 3)), dma((2, 2, NC)), dma((2, 2, NC)), dma((3,)), dma((2,)), dma((1,)), dma((1,)), dma((7 + 4 * NC,)),
        ]
        y, dx, n_a, dy_a, nr, ur, act, sact, dl = pl.pallas_call(
            line_kernel,
            name="line",
            out_shape=outs,
            in_specs=[any_, any_, vmem, vmem, vmem] + [any_] * 6,
            out_specs=[any_] * 9,
            scratch_shapes=scratch,
            compiler_params=pltpu.CompilerParams(collective_id=0, has_side_effects=True, vmem_limit_bytes=60 * 1024 * 1024),
        )(x, dy, prim.reshape(1, TL), alt.reshape(1, TL), wr, eg, eu, ed, sg, su, sd)

        gg, gu, gd = pl.pallas_call(
            grads_kernel,
            name="grads",
            grid=(EL,),
            out_shape=[sds((EL, D, W), F32), sds((EL, D, W), F32), sds((EL, W, D), F32)],
            in_specs=[pl.BlockSpec((CAP, D), lambda i: (i, 0)), pl.BlockSpec((CAP, D), lambda i: (i, 0)), pl.BlockSpec((3, CAP, W), lambda i: (0, i, 0))],
            out_specs=[pl.BlockSpec((1, D, W), lambda i: (i, 0, 0)), pl.BlockSpec((1, D, W), lambda i: (i, 0, 0)), pl.BlockSpec((1, W, D), lambda i: (i, 0, 0))],
            compiler_params=pltpu.CompilerParams(vmem_limit_bytes=40 * 1024 * 1024),
        )(nr, ur, act)
        g_sg = jnp.einsum("td,tf->df", n_a, sact[1], preferred_element_type=F32)
        g_su = jnp.einsum("td,tf->df", n_a, sact[2], preferred_element_type=F32)
        g_sd = jnp.einsum("tf,td->fd", sact[0], dy_a, preferred_element_type=F32)
        g_r = jnp.einsum("td,te->de", n_a, dl, preferred_element_type=F32)
        return y, dx, gg, gu, gd, g_sg, g_su, g_sd, g_r

    return jax.shard_map(step, mesh=mesh, in_specs=in_specs, out_specs=out_specs, check_vma=False)
```

```python
import functools

import jax
import jax.numpy as jnp
from jax import lax
from jax.experimental import pallas as pl
from jax.experimental.pallas import tpu as pltpu
from jax.sharding import PartitionSpec as P

EPS = 1e-5
F32 = jnp.float32
BF16 = jnp.bfloat16
MESH = pl.DeviceIdType.MESH
TL = 128
NEP = 4
T = TL * NEP
D = 1536
HD = D // 2
E = 40
EL = 10
CAP = 16
W = 128
NM = 18
MR = 32
NC = 4
CR = TL // NC


def dot(a, b):
    return jnp.dot(a, b, preferred_element_type=F32)


def dot_t(a, b):
    return lax.dot_general(a, b, (((1,), (1,)), ((), ())), preferred_element_type=F32)


def tdot(a, b):
    return lax.dot_general(a, b, (((0,), (0,)), ((), ())), preferred_element_type=F32)


def glu(a, b):
    return (a * jax.nn.sigmoid(a) * b).astype(BF16)


def glu_grads(dh, a, b):
    sig = jax.nn.sigmoid(a)
    d_gate = (dh * b * sig * (1.0 + a * (1.0 - sig))).astype(BF16)
    d_up = (dh * a * sig).astype(BF16)
    return d_gate, d_up


def line_kernel(
    x_h, dy_h, prim_v, alt_v, wr_v, wg_h, wu_h, wd_h, sg_h, su_h, sd_h,
    y_o, dx_o, n_o, dyo_o, nr_o, ur_o, act_o, sact_o, dl_o,
    x_a, dy_a, n_a, u_a, ids, wg, wu, wd, sg, su, sd, nr, ur, act, sact, dl,
    part, recv, o_all, dn_all, yb, dgb, pjb, tgt_v, g_v, df_v, dnr_v, ab,
    xl, wl, sl, ids_s, ids_r, xs, xr, zs, zr, es, er, ys, yr, dgs, dgr, pjs, pjr, outs,
):
    z = lax.axis_index("etp")
    e = lax.axis_index("ep")
    e_y, e_c, e_d = e ^ 2, e ^ 1, e ^ 3
    peers = (e_y, e_c, e_d)
    is_end = (z == 0) | (z == 3)
    is_mid = (z == 1) | (z == 2)
    hs = z // 3

    def rows(j):
        return pl.ds(pl.multiple_of(j * TL, TL), TL)

    mine = rows(e)
    lx = pltpu.make_async_copy(x_h, x_a.at[mine], xl.at[0])
    ldy = pltpu.make_async_copy(dy_h, dy_a.at[mine], xl.at[1])
    lx.start()
    ldy.start()
    shared_loads = [pltpu.make_async_copy(a, b, sl.at[k]) for k, (a, b) in enumerate(((sg_h, sg), (su_h, su), (sd_h, sd)))]
    for c in shared_loads:
        c.start()

    def wload(k, i):
        src, dst = ((wg_h, wg), (wu_h, wu), (wd_h, wd))[k]
        return pltpu.make_async_copy(src.at[i], dst.at[i], wl.at[k, i])

    ids[e] = jnp.zeros((8, TL), F32)
    ids[e, 0:1, :] = prim_v[...].astype(F32)
    ids[e, 1:2, :] = alt_v[...].astype(F32)

    barrier = pltpu.get_barrier_semaphore()
    for q in peers:
        pl.semaphore_signal(barrier, inc=1, device_id={"ep": q}, device_id_type=MESH)
    for k in range(1, 4):
        pl.semaphore_signal(barrier, inc=1, device_id={"etp": lax.rem(z + k, 4)}, device_id_type=MESH)
    pl.semaphore_wait(barrier, 6)

    def rcopy(src, dst, s, r, dev):
        return pltpu.make_async_remote_copy(src_ref=src, dst_ref=dst, send_sem=s, recv_sem=r, device_id=dev, device_id_type=MESH)

    ids_c = [rcopy(ids.at[e], ids.at[e], ids_s.at[k], ids_r.at[k], {"ep": peers[k]}) for k in range(3)]
    for c in ids_c:
        c.start()
    lx.wait()
    x_c, relays = [], []
    for k, buf in enumerate((x_a, dy_a)):
        if k == 1:
            ldy.wait()
        pair = [
            rcopy(buf.at[mine], buf.at[mine], xs.at[k, 0], xr.at[k, 0], {"ep": e_y}),
            rcopy(buf.at[mine], buf.at[mine], xs.at[k, 1], xr.at[k, 1], {"ep": e_c}),
        ]
        for c in pair:
            c.start()
        x_c.append(pair)
        relays.append(rcopy(buf.at[rows(e_y)], buf.at[rows(e_y)], xs.at[k, 2], xr.at[k, 2], {"ep": e_c}))

    def load_body(i, _):
        for k in range(3):
            wload(k, i).start()
        return 0

    lax.fori_loop(0, EL, load_body, 0)

    def line_copy(d, m):
        return rcopy(part.at[d, m], recv.at[d, m], zs.at[d, m], zr.at[d, m], {"etp": jnp.clip(z - 1 + 2 * d, 0, 3)})

    def source_send(m):
        @pl.when(z == 3)
        def _():
            line_copy(0, m).start()

        @pl.when(z == 0)
        def _():
            line_copy(1, m).start()

    def take(d, m):
        line_copy(d, m).wait_recv()
        part[d, m] = part[d, m] + recv[d, m]

    def forward(hop, m):
        @pl.when(is_mid)
        def _():
            d = (2 - z) if hop == 1 else (z - 1)
            take(d, m)
            line_copy(d, m).start()

    def norm(xw):
        inv = lax.rsqrt(jnp.mean(xw * xw, axis=1, keepdims=True) + EPS)
        return inv, (xw * inv).astype(BF16)

    for c in shared_loads:
        c.wait()

    def shared_acts(n, dy):
        a = dot(n, sg[...])
        b = dot(n, su[...])
        h = glu(a, b)
        dg_, du_ = glu_grads(dot_t(dy, sd[...]), a, b)
        return h, dg_, du_

    _, n_own = norm(x_a[mine, :].astype(F32))
    h_s, da_s, db_s = shared_acts(n_own, dy_a[mine, :])
    s_part = dot(h_s, sd[...])
    for k in range(4):
        part[0, k] = s_part[k * MR : (k + 1) * MR, :HD]
        part[1, k] = s_part[k * MR : (k + 1) * MR, HD:]
    dns_part = dot_t(da_s, sg[...]) + dot_t(db_s, su[...])
    for k in range(4):
        part[0, 4 + k] = dns_part[k * MR : (k + 1) * MR, :HD]
        part[1, 4 + k] = dns_part[k * MR : (k + 1) * MR, HD:]
    for m in range(8):
        source_send(m)

    forward(1, 0)
    forward(1, 1)
    forward(1, 2)
    forward(2, 0)

    for c in ids_c:
        c.wait_recv()
    x_c[0][0].wait_recv()
    relays[0].start()
    x_c[0][1].wait_recv()
    relays[0].wait_recv()

    def norm_body(j, _):
        _, n = norm(x_a[rows(j), :].astype(F32))
        n_a[rows(j), :] = n
        return 0

    lax.fori_loop(0, NEP, norm_body, 0)
    forward(1, 3)
    forward(2, 1)

    logits = dot_t(n_a[...], wr_v[...])
    ex = jnp.exp(logits - jnp.max(logits, axis=1, keepdims=True))
    probs = ex / jnp.sum(ex, axis=1, keepdims=True)
    cols = []
    for j in range(NEP):
        block = jnp.concatenate([ids[j], jnp.zeros((TL - 8, TL), F32)], axis=0)
        cols.append(jnp.transpose(block)[:, 0:2])
    idc = jnp.concatenate(cols, axis=0)
    prim, alt = idc[:, 0:1], idc[:, 1:2]
    iota_e = lax.broadcasted_iota(jnp.int32, (T, E), 1).astype(F32)
    one_p = jnp.where(prim == iota_e, 1.0, 0.0)
    earlier = jnp.where(
        lax.broadcasted_iota(jnp.int32, (T, T), 0) > lax.broadcasted_iota(jnp.int32, (T, T), 1), 1.0, 0.0
    ).astype(BF16)
    rank = jnp.sum(dot(earlier, one_p.astype(BF16)) * one_p, axis=1, keepdims=True)
    over = jnp.where(rank < CAP, 0.0, 1.0)
    kept = jnp.minimum(jnp.sum(one_p, axis=0, keepdims=True), float(CAP))
    one_a = jnp.where(alt == iota_e, 1.0, 0.0) * over
    slot_a = jnp.sum((dot(earlier, one_a.astype(BF16)) + kept) * one_a, axis=1, keepdims=True)
    keep_a = over * jnp.where(slot_a < CAP, 1.0, 0.0)
    one_s = one_p * (1.0 - over) + one_a * keep_a
    slot = (1.0 - over) * rank + keep_a * slot_a
    eid = jnp.sum(one_s * iota_e, axis=1, keepdims=True)
    has = (1.0 - over) + keep_a
    tgt_v[...] = jnp.where(has > 0.5, eid * CAP + slot, -1.0)
    g_v[...] = jnp.sum(probs * one_s, axis=1, keepdims=True)
    df_v[...] = one_s - probs

    base = (e * (EL * CAP)).astype(F32)
    pick = jnp.where(
        tgt_v[...] - base == lax.broadcasted_iota(jnp.int32, (T, EL * CAP), 1).astype(F32), 1.0, 0.0
    ).astype(BF16)
    nr[...] = tdot(pick, n_a[...]).astype(BF16)
    forward(1, 4)
    forward(2, 2)
    forward(1, 5)
    forward(2, 3)

    def fwd_pair(k, _):
        for half in range(2):
            i = 2 * k + half
            for w in range(3):
                wload(w, i).wait()
            sl16 = pl.ds(pl.multiple_of(i * CAP, CAP), CAP)
            n_i = nr[sl16, :]
            a = dot(n_i, wg[i])
            b = dot(n_i, wu[i])
            h = glu(a, b)
            ab[0, sl16, :] = a
            ab[1, sl16, :] = b
            act[0, sl16, :] = h
            o = dot(h, wd[i])
            r16 = slice(half * CAP, (half + 1) * CAP)
            part[0, 8 + k, r16, :] = o[:, :HD]
            part[1, 8 + k, r16, :] = o[:, HD:]
        source_send(8 + k)
        return 0

    lax.fori_loop(0, EL // 2, fwd_pair, 0)
    forward(1, 6)
    forward(2, 4)
    forward(1, 7)
    forward(2, 5)

    x_c[1][0].wait_recv()
    relays[1].start()
    x_c[1][1].wait_recv()
    relays[1].wait_recv()

    def u_body(j, _):
        u_a[rows(j), :] = (g_v[rows(j), :] * dy_a[rows(j), :].astype(F32)).astype(BF16)
        return 0

    lax.fori_loop(0, NEP, u_body, 0)
    ur[...] = tdot(pick, u_a[...]).astype(BF16)

    def pair_body(k, _):
        for half in range(2):
            i = 2 * k + half
            sl16 = pl.ds(pl.multiple_of(i * CAP, CAP), CAP)
            da, db = glu_grads(dot_t(ur[sl16, :], wd[i]), ab[0, sl16, :], ab[1, sl16, :])
            act[1, sl16, :] = da
            act[2, sl16, :] = db
            r16 = slice(half * CAP, (half + 1) * CAP)
            dn = dot_t(da, wg[i]) + dot_t(db, wu[i])
            part[0, 13 + k, r16, :] = dn[:, :HD]
            part[1, 13 + k, r16, :] = dn[:, HD:]
        source_send(13 + k)
        return 0

    lax.fori_loop(0, EL // 2, pair_body, 0)
    stores = [
        pltpu.make_async_copy(n_a, n_o, outs.at[0]),
        pltpu.make_async_copy(dy_a, dyo_o, outs.at[1]),
        pltpu.make_async_copy(nr, nr_o, outs.at[2]),
        pltpu.make_async_copy(ur, ur_o, outs.at[3]),
        pltpu.make_async_copy(act, act_o, outs.at[4]),
    ]
    for c in stores:
        c.start()

    def fwd_body(m, _):
        forward(1, m)
        forward(2, m - 2)
        return 0

    lax.fori_loop(8, NM, fwd_body, 0)
    forward(2, NM - 2)
    forward(2, NM - 1)

    def sact_body(j, _):
        h, da, db = shared_acts(n_a[rows(j), :], dy_a[rows(j), :])
        sact[0, rows(j), :] = h
        sact[1, rows(j), :] = da
        sact[2, rows(j), :] = db
        return 0

    lax.fori_loop(0, NEP, sact_body, 0)
    st = pltpu.make_async_copy(sact, sact_o, outs.at[5])
    st.start()
    stores.append(st)

    def exchange(t, k, p):
        buf = (o_all, dn_all)[t]
        return rcopy(buf.at[e, k], buf.at[e, k], es.at[t, k, p], er.at[t, k, p], {"ep": peers[p]})

    lanes = pl.ds(pl.multiple_of(hs * HD, 128), HD)

    def place(n_rows, start):
        t_col = tgt_v[pl.ds(start, n_rows), :]
        return jnp.where(
            t_col == lax.broadcasted_iota(jnp.int32, (n_rows, E * CAP), 1).astype(F32), 1.0, 0.0
        ).astype(BF16)

    def col_to_row(col):
        return jnp.transpose(jnp.broadcast_to(col, (TL, TL)))[0:1, :]

    def dg_copy(h, k):
        return rcopy(dgb.at[h], dgb.at[h], dgs.at[k], dgr.at[h], {"etp": lax.rem(z + k + 1, 4)})

    def pj_copy():
        return rcopy(pjb.at[hs], pjb.at[hs], pjs.at[0], pjr.at[0], {"etp": 3 - z})

    def end_take(m, _):
        take(hs, m)
        return 0

    def end_take_o(k, _):
        take(hs, 8 + k)
        o_all[e, k] = part[hs, 8 + k].astype(BF16)
        for p in range(3):
            exchange(0, k, p).start()
        return 0

    def end_take_dn(k, _):
        take(hs, 13 + k)
        dn_all[e, k] = part[hs, 13 + k].astype(BF16)
        for p in range(3):
            exchange(1, k, p).start()
        return 0

    def wait_exchange(t):
        def body(k, _):
            for p in range(3):
                exchange(t, k, p).wait_recv()
            return 0

        lax.fori_loop(0, EL // 2, body, 0)

    def relay_copy(t, h, c):
        return rcopy(yb.at[t, h, c], yb.at[t, h, c], ys.at[t, h, c], yr.at[t, h, c], {"etp": jnp.clip(z + 1 - 2 * h, 0, 3)})

    def relay_start(t):
        for c in range(NC):
            relay_copy(t, hs, c).start()

    @pl.when(is_end)
    def _():
        lax.fori_loop(0, 8, end_take, 0)
        lax.fori_loop(0, EL // 2, end_take_o, 0)
        wait_exchange(0)
        o_flat = o_all[...].reshape(E * CAP, HD)
        for j in range(NEP):
            tok = dot(place(TL, j * TL), o_flat)
            prod = dy_a[j * TL : (j + 1) * TL, lanes].astype(F32) * tok
            dgb[hs, 0:1, j * TL : (j + 1) * TL] = col_to_row(jnp.sum(prod, axis=1, keepdims=True))
        for k in range(3):
            dg_copy(hs, k).start()
        tok = dot(place(TL, pl.multiple_of(e * TL, TL)), o_flat)
        s_own = part[hs, 0:4].reshape(TL, HD)
        y = (x_a[mine, lanes].astype(F32) + s_own + g_v[mine, :] * tok).astype(BF16)
        for c in range(NC):
            yb[0, hs, c] = y[c * CR : (c + 1) * CR, :]
        relay_start(0)

    @pl.when(z != 0)
    def _():
        dg_copy(0, 0).wait_recv()

    @pl.when(z != 3)
    def _():
        dg_copy(1, 0).wait_recv()

    for j in range(NEP):
        row = dgb[0, 0:1, j * TL : (j + 1) * TL] + dgb[1, 0:1, j * TL : (j + 1) * TL]
        dg_col = jnp.transpose(jnp.broadcast_to(row, (TL, TL)))[:, 0:1]
        sl_j = slice(j * TL, (j + 1) * TL)
        dl[sl_j, :] = (dg_col * g_v[sl_j, :] * df_v[sl_j, :]).astype(BF16)
    st = pltpu.make_async_copy(dl, dl_o, outs.at[6])
    st.start()
    stores.append(st)

    def relay_wait(t, h, c):
        relay_copy(t, h, c).wait_recv()

    def relay_through(t):
        def hop(n, c):
            h = (z - 1) if n == 1 else (2 - z)
            relay_wait(t, h, c)
            relay_copy(t, h, c).start()

        @pl.when(is_mid)
        def _():
            for c in range(NC + 2):
                if c < NC:
                    hop(1, c)
                if c >= 2:
                    hop(2, c - 2)

        @pl.when(is_end)
        def _():
            for c in range(NC):
                relay_wait(t, 1 - hs, c)

    @pl.when(is_mid)
    def _():
        relay_through(0)

    @pl.when(is_end)
    def _():
        dn_r = dot(dl[mine, :], wr_v[...])
        dnr_v[0] = dn_r[:, :HD]
        dnr_v[1] = dn_r[:, HD:]
        lax.fori_loop(0, EL // 2, end_take_dn, 0)
        wait_exchange(1)
        tok = dot(place(TL, pl.multiple_of(e * TL, TL)), dn_all[...].reshape(E * CAP, HD))
        dn = part[hs, 4:8].reshape(TL, HD) + dnr_v[hs] + tok
        dnr_v[hs] = dn
        xh = x_a[mine, lanes].astype(F32)
        pjb[hs, 0:1, :] = col_to_row(jnp.sum(dn * xh, axis=1, keepdims=True))
        pj_copy().start()
        inv, _ = norm(x_a[mine, :].astype(F32))
        pj_copy().wait_recv()
        row = pjb[0, 0:1, :] + pjb[1, 0:1, :]
        proj = jnp.transpose(jnp.broadcast_to(row, (TL, TL)))[:, 0:1] * (1.0 / D)
        dx = (dy_a[mine, lanes].astype(F32) + inv * dnr_v[hs] - x_a[mine, lanes].astype(F32) * (inv * inv * inv) * proj).astype(BF16)
        for c in range(NC):
            yb[1, hs, c] = dx[c * CR : (c + 1) * CR, :]
        relay_start(1)

    @pl.when(is_end)
    def _():
        relay_through(0)

    def out_copies(t, out):
        cs = []
        for h in range(2):
            for c in range(NC):
                cs.append(pltpu.make_async_copy(yb.at[t, h, c], out.at[pl.ds(c * CR, CR), pl.ds(h * HD, HD)], outs.at[7 + t * 2 * NC + h * NC + c]))
        return cs

    oc = out_copies(0, y_o)
    for c in oc:
        c.start()
    stores += oc
    relay_through(1)
    oc = out_copies(1, dx_o)
    for c in oc:
        c.start()
    stores += oc

    for c in ids_c:
        c.wait_send()
    for k in range(2):
        for c in x_c[k]:
            c.wait_send()
        relays[k].wait_send()

    def line_drain(m, _):
        @pl.when(z != 0)
        def _():
            line_copy(0, m).wait_send()

        @pl.when(z != 3)
        def _():
            line_copy(1, m).wait_send()

        return 0

    lax.fori_loop(0, NM, line_drain, 0)

    @pl.when(is_end)
    def _():
        def drain(k, _):
            for t in range(2):
                for p in range(3):
                    exchange(t, k, p).wait_send()
            return 0

        lax.fori_loop(0, EL // 2, drain, 0)
        for k in range(3):
            dg_copy(hs, k).wait_send()
        pj_copy().wait_send()

    for t in range(2):
        for c in range(NC):
            @pl.when(z != 3)
            def _(t=t, c=c):
                relay_copy(t, 0, c).wait_send()

            @pl.when(z != 0)
            def _(t=t, c=c):
                relay_copy(t, 1, c).wait_send()

    for c in stores:
        c.wait()


def grads_kernel(nr, ur, act, n_h, dy_h, sact, dl, y_h, dx_h, gg, gu, gd, gsg_h, gsu_h, gsd_h, gr_h, yo_h, dxo_h, n, dy, yx, gs, gsd, gr, li, so):
    i = pl.program_id(0)
    loads = [pltpu.make_async_copy(a, b, li.at[k]) for k, (a, b) in enumerate(((n_h, n), (dy_h, dy), (y_h, yx.at[0]), (dx_h, yx.at[1])))]
    pairs = ((gs.at[0], gsg_h), (gs.at[1], gsu_h), (gsd, gsd_h), (gr, gr_h), (yx.at[0], yo_h), (yx.at[1], dxo_h))
    stores = [pltpu.make_async_copy(a, b, so.at[k]) for k, (a, b) in enumerate(pairs)]

    @pl.when(i == 0)
    def _():
        for c in loads:
            c.start()

    @pl.when(i == 2)
    def _():
        for c in loads:
            c.wait()
        for c in stores[4:]:
            c.start()
        gs[0] = tdot(n[...], sact[1])
        stores[0].start()

    @pl.when(i == 3)
    def _():
        gs[1] = tdot(n[...], sact[2])
        stores[1].start()

    @pl.when(i == 4)
    def _():
        gsd[...] = tdot(sact[0], dy[...])
        stores[2].start()

    @pl.when(i == 5)
    def _():
        gr[...] = tdot(dl[...], n[...])
        stores[3].start()

    @pl.when(i == EL - 1)
    def _():
        for c in stores:
            c.wait()

    gg[0] = tdot(nr[...], act[1])
    gu[0] = tdot(nr[...], act[2])
    gd[0] = tdot(act[0], ur[...])


def solution(mesh):
    tok = P(("dp", "ep"), None)
    ids = P(("dp", "ep"))
    in_specs = (tok, tok, ids, ids, P(None, None), P("ep", None, "etp"), P("ep", None, "etp"), P("ep", "etp", None), P(None, "etp"), P(None, "etp"), P("etp", None))
    out_specs = (tok, tok, P(("dp", "ep"), None, "etp"), P(("dp", "ep"), None, "etp"), P(("dp", "ep"), "etp", None), P("dp", "etp"), P("dp", "etp"), P(("dp", "etp"), None), P("dp", None))
    any_ = pl.BlockSpec(memory_space=pl.ANY)
    vmem = pl.BlockSpec(memory_space=pltpu.VMEM)
    dma = pltpu.SemaphoreType.DMA

    def sds(shape, dtype):
        return jax.ShapeDtypeStruct(shape, dtype)

    def step(x, dy, prim, alt, wr, eg, eu, ed, sg, su, sd):
        outs = [
            sds((TL, D), BF16), sds((TL, D), BF16), sds((T, D), BF16), sds((T, D), BF16),
            sds((EL * CAP, D), BF16), sds((EL * CAP, D), BF16), sds((3, EL * CAP, W), BF16), sds((3, T, W), BF16), sds((T, E), BF16),
        ]
        V = pltpu.VMEM
        scratch = [
            V((T, D), BF16), V((T, D), BF16), V((T, D), BF16), V((T, D), BF16), V((NEP, 8, TL), F32),
            V((EL, D, W), BF16), V((EL, D, W), BF16), V((EL, W, D), BF16), V((D, W), BF16), V((D, W), BF16), V((W, D), BF16),
            V((EL * CAP, D), BF16), V((EL * CAP, D), BF16), V((3, EL * CAP, W), BF16), V((3, T, W), BF16), V((T, E), BF16),
            V((2, NM, MR, HD), F32), V((2, NM, MR, HD), F32), V((NEP, EL // 2, MR, HD), BF16), V((NEP, EL // 2, MR, HD), BF16),
            V((2, 2, NC, CR, HD), BF16), V((2, 8, T), F32), V((2, 8, TL), F32), V((T, 1), F32), V((T, 1), F32), V((T, E), F32), V((2, TL, HD), F32), V((2, EL * CAP, W), F32),
            dma((2,)), dma((3, EL)), dma((3,)), dma((3,)), dma((3,)), dma((2, 3)), dma((2, 3)), dma((2, NM)), dma((2, NM)),
            dma((2, EL // 2, 3)), dma((2, EL // 2, 3)), dma((2, 2, NC)), dma((2, 2, NC)), dma((3,)), dma((2,)), dma((1,)), dma((1,)), dma((7 + 4 * NC,)),
        ]
        y, dx, n_a, dy_a, nr, ur, act, sact, dl = pl.pallas_call(
            line_kernel,
            name="line",
            out_shape=outs,
            in_specs=[any_, any_, vmem, vmem, vmem] + [any_] * 6,
            out_specs=[any_] * 9,
            scratch_shapes=scratch,
            compiler_params=pltpu.CompilerParams(collective_id=0, has_side_effects=True, vmem_limit_bytes=60 * 1024 * 1024),
        )(x, dy, prim.reshape(1, TL), alt.reshape(1, TL), wr.T, eg, eu, ed, sg, su, sd)

        gg, gu, gd, g_sg, g_su, g_sd, g_r, y, dx = pl.pallas_call(
            grads_kernel,
            name="grads",
            grid=(EL,),
            out_shape=[
                sds((EL, D, W), F32), sds((EL, D, W), F32), sds((EL, W, D), F32),
                sds((D, W), F32), sds((D, W), F32), sds((W, D), F32), sds((E, D), F32), sds((TL, D), BF16), sds((TL, D), BF16),
            ],
            in_specs=[pl.BlockSpec((CAP, D), lambda i: (i, 0)), pl.BlockSpec((CAP, D), lambda i: (i, 0)), pl.BlockSpec((3, CAP, W), lambda i: (0, i, 0)), any_, any_, vmem, vmem, any_, any_],
            out_specs=[pl.BlockSpec((1, D, W), lambda i: (i, 0, 0)), pl.BlockSpec((1, D, W), lambda i: (i, 0, 0)), pl.BlockSpec((1, W, D), lambda i: (i, 0, 0))] + [any_] * 6,
            scratch_shapes=[V((T, D), BF16), V((T, D), BF16), V((2, TL, D), BF16), V((2, D, W), F32), V((W, D), F32), V((E, D), F32), dma((4,)), dma((6,))],
            compiler_params=pltpu.CompilerParams(vmem_limit_bytes=60 * 1024 * 1024),
        )(nr, ur, act, n_a, dy_a, sact, dl, y, dx)
        return y, dx, gg, gu, gd, g_sg, g_su, g_sd, g_r.T

    return jax.shard_map(step, mesh=mesh, in_specs=in_specs, out_specs=out_specs, check_vma=False)
```

```python
import functools

import jax
import jax.numpy as jnp
from jax import lax
from jax.experimental import pallas as pl
from jax.experimental.pallas import tpu as pltpu
from jax.sharding import PartitionSpec as P

EPS = 1e-5
F32 = jnp.float32
BF16 = jnp.bfloat16
MESH = pl.DeviceIdType.MESH
TL = 128
NEP = 4
T = TL * NEP
D = 1536
HD = D // 2
E = 40
EL = 10
CAP = 16
W = 128
MR = 32
NS = TL // MR
PE = MR // CAP
NP = EL // PE
O0 = 2 * NS
N0 = O0 + NP
NM = N0 + NP
NC = 4
CR = TL // NC


def dot(a, b):
    return jnp.dot(a, b, preferred_element_type=F32)


def dot_t(a, b):
    return lax.dot_general(a, b, (((1,), (1,)), ((), ())), preferred_element_type=F32)


def tdot(a, b):
    return lax.dot_general(a, b, (((0,), (0,)), ((), ())), preferred_element_type=F32)


def glu(a, b):
    return (a * jax.nn.sigmoid(a) * b).astype(BF16)


def glu_grads(dh, a, b):
    sig = jax.nn.sigmoid(a)
    d_gate = (dh * b * sig * (1.0 + a * (1.0 - sig))).astype(BF16)
    d_up = (dh * a * sig).astype(BF16)
    return d_gate, d_up


def line_kernel(
    x_h, dy_h, prim_v, alt_v, wr_v, wg_h, wu_h, wd_h, sg_h, su_h, sd_h,
    y_o, dx_o, nr_o, ur_o, act_o, gs_o, gsd_o, gr_o,
    x_a, dy_a, n_a, u_a, ids, wg, wu, wd, sg, su, sd, nr, ur, act, sact, dl, gs, gsd, gr,
    part, recv, o_all, dn_all, yb, dxb, dgb, pjb, tgt_v, g_v, df_v, dnr_v, ab,
    xl, wl, sl, ids_s, ids_r, xs, xr, zs, zr, es, er, ys, yr, dgs, dgr, pjs, pjr, outs,
):
    z = lax.axis_index("etp")
    e = lax.axis_index("ep")
    e_y, e_c, e_d = e ^ 2, e ^ 1, e ^ 3
    peers = (e_y, e_c, e_d)
    is_end = (z == 0) | (z == 3)
    is_mid = (z == 1) | (z == 2)
    hs = z // 3

    def rows(j):
        return pl.ds(pl.multiple_of(j * TL, TL), TL)

    mine = rows(e)
    lx = pltpu.make_async_copy(x_h, x_a.at[mine], xl.at[0])
    ldy = pltpu.make_async_copy(dy_h, dy_a.at[mine], xl.at[1])
    lx.start()
    ldy.start()
    shared_loads = [pltpu.make_async_copy(a, b, sl.at[k]) for k, (a, b) in enumerate(((sg_h, sg), (su_h, su), (sd_h, sd)))]
    for c in shared_loads:
        c.start()

    def wload(k, i):
        src, dst = ((wg_h, wg), (wu_h, wu), (wd_h, wd))[k]
        return pltpu.make_async_copy(src.at[i], dst.at[i], wl.at[k, i])

    ids[e] = jnp.zeros((8, TL), F32)
    ids[e, 0:1, :] = prim_v[...].astype(F32)
    ids[e, 1:2, :] = alt_v[...].astype(F32)

    barrier = pltpu.get_barrier_semaphore()
    for q in peers:
        pl.semaphore_signal(barrier, inc=1, device_id={"ep": q}, device_id_type=MESH)
    for k in range(1, 4):
        pl.semaphore_signal(barrier, inc=1, device_id={"etp": lax.rem(z + k, 4)}, device_id_type=MESH)
    pl.semaphore_wait(barrier, 6)

    def rcopy(src, dst, s, r, dev):
        return pltpu.make_async_remote_copy(src_ref=src, dst_ref=dst, send_sem=s, recv_sem=r, device_id=dev, device_id_type=MESH)

    ids_c = [rcopy(ids.at[e], ids.at[e], ids_s.at[k], ids_r.at[k], {"ep": peers[k]}) for k in range(3)]
    for c in ids_c:
        c.start()
    lx.wait()
    x_c, relays = [], []
    for k, buf in enumerate((x_a, dy_a)):
        if k == 1:
            ldy.wait()
        pair = [
            rcopy(buf.at[mine], buf.at[mine], xs.at[k, 0], xr.at[k, 0], {"ep": e_y}),
            rcopy(buf.at[mine], buf.at[mine], xs.at[k, 1], xr.at[k, 1], {"ep": e_c}),
        ]
        for c in pair:
            c.start()
        x_c.append(pair)
        relays.append(rcopy(buf.at[rows(e_y)], buf.at[rows(e_y)], xs.at[k, 2], xr.at[k, 2], {"ep": e_c}))

    def load_body(i, _):
        for k in range(3):
            wload(k, i).start()
        return 0

    lax.fori_loop(0, EL, load_body, 0)

    def line_copy(d, m):
        return rcopy(part.at[d, m], recv.at[d, m], zs.at[d, m], zr.at[d, m], {"etp": jnp.clip(z - 1 + 2 * d, 0, 3)})

    def source_send(m):
        @pl.when(z == 3)
        def _():
            line_copy(0, m).start()

        @pl.when(z == 0)
        def _():
            line_copy(1, m).start()

    def take(d, m):
        line_copy(d, m).wait_recv()
        part[d, m] = part[d, m] + recv[d, m]

    def forward(hop, m):
        @pl.when(is_mid)
        def _():
            d = (2 - z) if hop == 1 else (z - 1)
            take(d, m)
            line_copy(d, m).start()

    def norm(xw):
        inv = lax.rsqrt(jnp.mean(xw * xw, axis=1, keepdims=True) + EPS)
        return inv, (xw * inv).astype(BF16)

    for c in shared_loads:
        c.wait()

    def shared_acts(n, dy):
        a = dot(n, sg[...])
        b = dot(n, su[...])
        h = glu(a, b)
        dg_, du_ = glu_grads(dot_t(dy, sd[...]), a, b)
        return h, dg_, du_

    _, n_own = norm(x_a[mine, :].astype(F32))
    h_s, da_s, db_s = shared_acts(n_own, dy_a[mine, :])
    s_part = dot(h_s, sd[...])
    for k in range(NS):
        part[0, k] = s_part[k * MR : (k + 1) * MR, :HD]
        part[1, k] = s_part[k * MR : (k + 1) * MR, HD:]
    dns_part = dot_t(da_s, sg[...]) + dot_t(db_s, su[...])
    for k in range(NS):
        part[0, NS + k] = dns_part[k * MR : (k + 1) * MR, :HD]
        part[1, NS + k] = dns_part[k * MR : (k + 1) * MR, HD:]
    for m in range(O0):
        source_send(m)

    def forwards(hop1, hop2):
        n1, n2 = len(hop1), len(hop2)
        for i in range(max(n1, n2)):
            if i < n1:
                forward(1, hop1[i])
            if i < n2:
                forward(2, hop2[i])

    forwards(range(0, 3), range(0, 1))

    for c in ids_c:
        c.wait_recv()
    x_c[0][0].wait_recv()
    relays[0].start()
    x_c[0][1].wait_recv()
    relays[0].wait_recv()

    def norm_body(j, _):
        _, n = norm(x_a[rows(j), :].astype(F32))
        n_a[rows(j), :] = n
        return 0

    lax.fori_loop(0, NEP, norm_body, 0)
    forwards(range(3, 4), range(1, 2))

    logits = dot_t(n_a[...], wr_v[...])
    ex = jnp.exp(logits - jnp.max(logits, axis=1, keepdims=True))
    probs = ex / jnp.sum(ex, axis=1, keepdims=True)
    cols = []
    for j in range(NEP):
        block = jnp.concatenate([ids[j], jnp.zeros((TL - 8, TL), F32)], axis=0)
        cols.append(jnp.transpose(block)[:, 0:2])
    idc = jnp.concatenate(cols, axis=0)
    prim, alt = idc[:, 0:1], idc[:, 1:2]
    iota_e = lax.broadcasted_iota(jnp.int32, (T, E), 1).astype(F32)
    one_p = jnp.where(prim == iota_e, 1.0, 0.0)
    earlier = jnp.where(
        lax.broadcasted_iota(jnp.int32, (T, T), 0) > lax.broadcasted_iota(jnp.int32, (T, T), 1), 1.0, 0.0
    ).astype(BF16)
    rank = jnp.sum(dot(earlier, one_p.astype(BF16)) * one_p, axis=1, keepdims=True)
    over = jnp.where(rank < CAP, 0.0, 1.0)
    kept = jnp.minimum(jnp.sum(one_p, axis=0, keepdims=True), float(CAP))
    one_a = jnp.where(alt == iota_e, 1.0, 0.0) * over
    slot_a = jnp.sum((dot(earlier, one_a.astype(BF16)) + kept) * one_a, axis=1, keepdims=True)
    keep_a = over * jnp.where(slot_a < CAP, 1.0, 0.0)
    one_s = one_p * (1.0 - over) + one_a * keep_a
    slot = (1.0 - over) * rank + keep_a * slot_a
    eid = jnp.sum(one_s * iota_e, axis=1, keepdims=True)
    has = (1.0 - over) + keep_a
    tgt_v[...] = jnp.where(has > 0.5, eid * CAP + slot, -1.0)
    g_v[...] = jnp.sum(probs * one_s, axis=1, keepdims=True)
    df_v[...] = one_s - probs

    base = (e * (EL * CAP)).astype(F32)
    pick = jnp.where(
        tgt_v[...] - base == lax.broadcasted_iota(jnp.int32, (T, EL * CAP), 1).astype(F32), 1.0, 0.0
    ).astype(BF16)
    nr[...] = tdot(pick, n_a[...]).astype(BF16)
    forwards(range(4, 6), range(2, 4))

    def expert_forward(k, _):
        for half in range(PE):
            i = PE * k + half
            for w in range(3):
                wload(w, i).wait()
            sl16 = pl.ds(pl.multiple_of(i * CAP, CAP), CAP)
            n_i = nr[sl16, :]
            a = dot(n_i, wg[i])
            b = dot(n_i, wu[i])
            h = glu(a, b)
            ab[0, sl16, :] = a
            ab[1, sl16, :] = b
            act[0, sl16, :] = h
            o = dot(h, wd[i])
            r16 = slice(half * CAP, (half + 1) * CAP)
            part[0, O0 + k, r16, :] = o[:, :HD]
            part[1, O0 + k, r16, :] = o[:, HD:]
        source_send(O0 + k)
        return 0

    lax.fori_loop(0, NP, expert_forward, 0)
    forwards(range(6, 8), range(4, 6))

    x_c[1][0].wait_recv()
    relays[1].start()
    x_c[1][1].wait_recv()
    relays[1].wait_recv()

    def u_body(j, _):
        u_a[rows(j), :] = (g_v[rows(j), :] * dy_a[rows(j), :].astype(F32)).astype(BF16)
        return 0

    lax.fori_loop(0, NEP, u_body, 0)
    ur[...] = tdot(pick, u_a[...]).astype(BF16)

    def expert_backward(k, _):
        for half in range(PE):
            i = PE * k + half
            sl16 = pl.ds(pl.multiple_of(i * CAP, CAP), CAP)
            da, db = glu_grads(dot_t(ur[sl16, :], wd[i]), ab[0, sl16, :], ab[1, sl16, :])
            act[1, sl16, :] = da
            act[2, sl16, :] = db
            dn = dot_t(da, wg[i]) + dot_t(db, wu[i])
            r16 = slice(half * CAP, (half + 1) * CAP)
            part[0, N0 + k, r16, :] = dn[:, :HD]
            part[1, N0 + k, r16, :] = dn[:, HD:]
        source_send(N0 + k)
        forward(1, O0 + k)
        forward(2, O0 - 2 + k)
        return 0

    lax.fori_loop(0, NP, expert_backward, 0)
    stores = [
        pltpu.make_async_copy(nr, nr_o, outs.at[2]),
        pltpu.make_async_copy(ur, ur_o, outs.at[3]),
        pltpu.make_async_copy(act, act_o, outs.at[4]),
    ]
    for c in stores:
        c.start()

    def sact_body(j, _):
        h, da, db = shared_acts(n_a[rows(j), :], dy_a[rows(j), :])
        sact[0, rows(j), :] = h
        sact[1, rows(j), :] = da
        sact[2, rows(j), :] = db
        return 0

    def shared_grads(c, _):
        cols = pl.ds(pl.multiple_of(c * W, W), W)
        n_c = n_a[:, cols]
        gs[0, cols, :] = tdot(n_c, sact[1])
        gs[1, cols, :] = tdot(n_c, sact[2])
        gsd[:, cols] = tdot(sact[0], dy_a[:, cols])
        return 0

    def piece_a(k):
        sact_body(2 * k, 0)
        sact_body(2 * k + 1, 0)

    def piece_b(k):
        lax.fori_loop(4 * k - 8, 4 * k - 4, shared_grads, 0)

    def message_loop(step):
        def with_piece(piece):
            def body(k, _):
                step(k)
                piece(k)
                return 0

            return body

        lax.fori_loop(0, 2, with_piece(piece_a), 0)
        lax.fori_loop(2, NP, with_piece(piece_b), 0)

    @pl.when(is_mid)
    def _():
        def step(k):
            forward(1, N0 + k)
            forward(2, N0 - 2 + k)

        message_loop(step)
        forward(2, NM - 2)
        forward(2, NM - 1)

    def exchange(t, k, p):
        buf = (o_all, dn_all)[t]
        return rcopy(buf.at[e, k], buf.at[e, k], es.at[t, k, p], er.at[t, k, p], {"ep": peers[p]})

    lanes = pl.ds(pl.multiple_of(hs * HD, 128), HD)

    def place(n_rows, start):
        t_col = tgt_v[pl.ds(start, n_rows), :]
        return jnp.where(
            t_col == lax.broadcasted_iota(jnp.int32, (n_rows, E * CAP), 1).astype(F32), 1.0, 0.0
        ).astype(BF16)

    def col_to_row(col):
        return jnp.transpose(jnp.broadcast_to(col, (TL, TL)))[0:1, :]

    def dg_copy(h, k):
        return rcopy(dgb.at[h], dgb.at[h], dgs.at[k], dgr.at[h], {"etp": lax.rem(z + k + 1, 4)})

    def pj_copy():
        return rcopy(pjb.at[hs], pjb.at[hs], pjs.at[0], pjr.at[0], {"etp": 3 - z})

    def end_take(m, _):
        take(hs, m)
        return 0

    def end_take_o(k, _):
        take(hs, O0 + k)
        o_all[e, k] = part[hs, O0 + k].astype(BF16)
        for p in range(3):
            exchange(0, k, p).start()
        return 0

    def end_take_dn(k, _):
        take(hs, N0 + k)
        dn_all[e, k] = part[hs, N0 + k].astype(BF16)
        for p in range(3):
            exchange(1, k, p).start()
        return 0

    def wait_exchange(t):
        def body(k, _):
            for p in range(3):
                exchange(t, k, p).wait_recv()
            return 0

        lax.fori_loop(0, NP, body, 0)

    def relay_copy(t, h, c):
        return rcopy(yb.at[t, h, c], yb.at[t, h, c], ys.at[t, h, c], yr.at[t, h, c], {"etp": jnp.clip(z + 1 - 2 * h, 0, 3)})

    def relay_start(t):
        for c in range(NC):
            relay_copy(t, hs, c).start()

    @pl.when(is_end)
    def _():
        lax.fori_loop(0, O0, end_take, 0)

        message_loop(lambda k: end_take_o(k, 0))
        lax.fori_loop(0, 2, end_take_dn, 0)
        wait_exchange(0)
        o_flat = o_all[...].reshape(E * CAP, HD)
        for j in range(NEP):
            tok = dot(place(TL, j * TL), o_flat)
            prod = dy_a[j * TL : (j + 1) * TL, lanes].astype(F32) * tok
            dgb[hs, 0:1, j * TL : (j + 1) * TL] = col_to_row(jnp.sum(prod, axis=1, keepdims=True))
        for k in range(3):
            dg_copy(hs, k).start()
        tok = dot(place(TL, pl.multiple_of(e * TL, TL)), o_flat)
        s_own = part[hs, 0:NS].reshape(TL, HD)
        y = (x_a[mine, lanes].astype(F32) + s_own + g_v[mine, :] * tok).astype(BF16)
        for c in range(NC):
            yb[0, hs, c] = y[c * CR : (c + 1) * CR, :]
        relay_start(0)
        lax.fori_loop(2, NP, end_take_dn, 0)

    late = [pltpu.make_async_copy(gs, gs_o, outs.at[0]), pltpu.make_async_copy(gsd, gsd_o, outs.at[1])]
    for c in late:
        c.start()
    stores += late

    @pl.when(z != 0)
    def _():
        dg_copy(0, 0).wait_recv()

    @pl.when(z != 3)
    def _():
        dg_copy(1, 0).wait_recv()

    for j in range(NEP):
        row = dgb[0, 0:1, j * TL : (j + 1) * TL] + dgb[1, 0:1, j * TL : (j + 1) * TL]
        dg_col = jnp.transpose(jnp.broadcast_to(row, (TL, TL)))[:, 0:1]
        sl_j = slice(j * TL, (j + 1) * TL)
        dl[sl_j, :] = (dg_col * g_v[sl_j, :] * df_v[sl_j, :]).astype(BF16)
    def router_grad():
        gr[...] = tdot(dl[...], n_a[...])

    def relay_wait(t, h, c):
        relay_copy(t, h, c).wait_recv()

    def relay_through(t):
        def hop(n, c):
            h = (z - 1) if n == 1 else (2 - z)
            relay_wait(t, h, c)
            relay_copy(t, h, c).start()

        @pl.when(is_mid)
        def _():
            for c in range(NC + 2):
                if c < NC:
                    hop(1, c)
                if c >= 2:
                    hop(2, c - 2)

        @pl.when(is_end)
        def _():
            for c in range(NC):
                relay_wait(t, 1 - hs, c)

    @pl.when(is_mid)
    def _():
        router_grad()
        relay_through(0)

    @pl.when(is_end)
    def _():
        dn_r = dot(dl[mine, :], wr_v[...])
        dnr_v[0] = dn_r[:, :HD]
        dnr_v[1] = dn_r[:, HD:]
        router_grad()
        wait_exchange(1)
        tok = dot(place(TL, pl.multiple_of(e * TL, TL)), dn_all[...].reshape(E * CAP, HD))
        dn = part[hs, NS:O0].reshape(TL, HD) + dnr_v[hs] + tok
        dnr_v[hs] = dn
        xh = x_a[mine, lanes].astype(F32)
        pjb[hs, 0:1, :] = col_to_row(jnp.sum(dn * xh, axis=1, keepdims=True))
        pj_copy().start()
        inv, _ = norm(x_a[mine, :].astype(F32))
        pj_copy().wait_recv()
        row = pjb[0, 0:1, :] + pjb[1, 0:1, :]
        proj = jnp.transpose(jnp.broadcast_to(row, (TL, TL)))[:, 0:1] * (1.0 / D)
        dx = (dy_a[mine, lanes].astype(F32) + inv * dnr_v[hs] - x_a[mine, lanes].astype(F32) * (inv * inv * inv) * proj).astype(BF16)
        dxb[...] = dx

    @pl.when(is_end)
    def _():
        relay_through(0)

    @pl.when(is_mid)
    def _():
        dxb[...] = jnp.zeros_like(dxb)

    st = pltpu.make_async_copy(gr, gr_o, outs.at[5])
    st.start()
    stores.append(st)

    def out_copies(t, out):
        cs = []
        for h in range(2):
            for c in range(NC):
                cs.append(pltpu.make_async_copy(yb.at[t, h, c], out.at[pl.ds(c * CR, CR), pl.ds(h * HD, HD)], outs.at[7 + t * 2 * NC + h * NC + c]))
        return cs

    oc = out_copies(0, y_o)
    for c in oc:
        c.start()
    stores += oc
    st = pltpu.make_async_copy(dxb, dx_o, outs.at[6])
    st.start()
    stores.append(st)

    for c in ids_c:
        c.wait_send()
    for k in range(2):
        for c in x_c[k]:
            c.wait_send()
        relays[k].wait_send()

    def line_drain(m, _):
        @pl.when(z != 0)
        def _():
            line_copy(0, m).wait_send()

        @pl.when(z != 3)
        def _():
            line_copy(1, m).wait_send()

        return 0

    lax.fori_loop(0, NM, line_drain, 0)

    @pl.when(is_end)
    def _():
        def drain(k, _):
            for t in range(2):
                for p in range(3):
                    exchange(t, k, p).wait_send()
            return 0

        lax.fori_loop(0, NP, drain, 0)
        for k in range(3):
            dg_copy(hs, k).wait_send()
        pj_copy().wait_send()

    for t in range(1):
        for c in range(NC):
            @pl.when(z != 3)
            def _(t=t, c=c):
                relay_copy(t, 0, c).wait_send()

            @pl.when(z != 0)
            def _(t=t, c=c):
                relay_copy(t, 1, c).wait_send()

    for c in stores:
        c.wait()


def grads_kernel(nr_h, ur_h, act_h, gs_h, gsd_h, gr_h, y_h, gg_o, gu_o, gd_o, gsg_o, gsu_o, gsd_o, gr_o, y_o, nr, ur, act, gs, gsd, gr, yv, gg, gu, gd, ri, ro, li, so):
    first = [pltpu.make_async_copy(a, b, ri.at[k]) for k, (a, b) in enumerate(((nr_h, nr), (ur_h, ur), (act_h, act)))]
    through = ((gs_h.at[0], gs.at[0], gsg_o), (gs_h.at[1], gs.at[1], gsu_o), (gsd_h, gsd, gsd_o), (gr_h, gr, gr_o), (y_h, yv, y_o))
    loads = [pltpu.make_async_copy(a, b, li.at[k]) for k, (a, b, _) in enumerate(through)]
    stores = [pltpu.make_async_copy(b, c, so.at[k]) for k, (_, b, c) in enumerate(through)]
    for c in first:
        c.start()
    for c in loads:
        c.start()
    for c in first:
        c.wait()

    def out(k, i):
        src, dst = ((gg, gg_o), (gu, gu_o), (gd, gd_o))[k]
        return pltpu.make_async_copy(src.at[i], dst.at[i], ro.at[k, i])

    def body(i, _):
        r = pl.ds(pl.multiple_of(i * CAP, CAP), CAP)
        n = nr[r, :]
        gg[i] = tdot(n, act[1, r, :])
        out(0, i).start()
        gu[i] = tdot(n, act[2, r, :])
        out(1, i).start()
        gd[i] = tdot(act[0, r, :], ur[r, :])
        out(2, i).start()
        return 0

    lax.fori_loop(0, EL, body, 0)
    for a, b in zip(loads, stores):
        a.wait()
        b.start()
    for c in stores:
        c.wait()

    def drain(i, _):
        for k in range(3):
            out(k, i).wait()
        return 0

    lax.fori_loop(0, EL, drain, 0)


def solution(mesh):
    tok = P(("dp", "ep"), None)
    ids = P(("dp", "ep"))
    in_specs = (tok, tok, ids, ids, P(None, None), P("ep", None, "etp"), P("ep", None, "etp"), P("ep", "etp", None), P(None, "etp"), P(None, "etp"), P("etp", None))
    out_specs = (tok, tok, P(("dp", "ep"), None, "etp"), P(("dp", "ep"), None, "etp"), P(("dp", "ep"), "etp", None), P("dp", "etp"), P("dp", "etp"), P(("dp", "etp"), None), P("dp", None))
    any_ = pl.BlockSpec(memory_space=pl.ANY)
    vmem = pl.BlockSpec(memory_space=pltpu.VMEM)
    dma = pltpu.SemaphoreType.DMA

    def sds(shape, dtype):
        return jax.ShapeDtypeStruct(shape, dtype)

    def step(x, dy, prim, alt, wr, eg, eu, ed, sg, su, sd):
        outs = [
            sds((TL, D), BF16), sds((TL, HD), BF16), sds((EL * CAP, D), BF16), sds((EL * CAP, D), BF16), sds((3, EL * CAP, W), BF16),
            sds((2, D, W), F32), sds((W, D), F32), sds((E, D), F32),
        ]
        V = pltpu.VMEM
        scratch = [
            V((T, D), BF16), V((T, D), BF16), V((T, D), BF16), V((T, D), BF16), V((NEP, 8, TL), F32),
            V((EL, D, W), BF16), V((EL, D, W), BF16), V((EL, W, D), BF16), V((D, W), BF16), V((D, W), BF16), V((W, D), BF16),
            V((EL * CAP, D), BF16), V((EL * CAP, D), BF16), V((3, EL * CAP, W), BF16), V((3, T, W), BF16), V((T, E), BF16), V((2, D, W), F32), V((W, D), F32), V((E, D), F32),
            V((2, NM, MR, HD), F32), V((2, NM, MR, HD), F32), V((NEP, NP, MR, HD), BF16), V((NEP, NP, MR, HD), BF16),
            V((1, 2, NC, CR, HD), BF16), V((TL, HD), BF16), V((2, 8, T), F32), V((2, 8, TL), F32), V((T, 1), F32), V((T, 1), F32), V((T, E), F32), V((2, TL, HD), F32), V((2, EL * CAP, W), F32),
            dma((2,)), dma((3, EL)), dma((3,)), dma((3,)), dma((3,)), dma((2, 3)), dma((2, 3)), dma((2, NM)), dma((2, NM)),
            dma((2, NP, 3)), dma((2, NP, 3)), dma((1, 2, NC)), dma((1, 2, NC)), dma((3,)), dma((2,)), dma((1,)), dma((1,)), dma((7 + 4 * NC,)),
        ]
        y, dxh, nr, ur, act, gs, gsd, gr = pl.pallas_call(
            line_kernel,
            name="line",
            out_shape=outs,
            in_specs=[any_, any_, vmem, vmem, vmem] + [any_] * 6,
            out_specs=[any_] * 8,
            scratch_shapes=scratch,
            compiler_params=pltpu.CompilerParams(collective_id=0, has_side_effects=True, vmem_limit_bytes=60 * 1024 * 1024),
        )(x, dy, prim.reshape(1, TL), alt.reshape(1, TL), wr.T, eg, eu, ed, sg, su, sd)

        across = lax.ppermute(dxh, "etp", [(0, 3), (3, 0)])
        far = lax.ppermute(dxh, "etp", [(0, 2), (3, 1)])
        near = lax.ppermute(dxh, "etp", [(0, 1), (3, 2)])
        gg, gu, gd, g_sg, g_su, g_sd, g_r, y = pl.pallas_call(
            grads_kernel,
            name="grads",
            out_shape=[
                sds((EL, D, W), F32), sds((EL, D, W), F32), sds((EL, W, D), F32),
                sds((D, W), F32), sds((D, W), F32), sds((W, D), F32), sds((E, D), F32), sds((TL, D), BF16),
            ],
            in_specs=[any_] * 7,
            out_specs=[any_] * 8,
            scratch_shapes=[
                V((EL * CAP, D), BF16), V((EL * CAP, D), BF16), V((3, EL * CAP, W), BF16), V((2, D, W), F32), V((W, D), F32), V((E, D), F32), V((TL, D), BF16),
                V((EL, D, W), F32), V((EL, D, W), F32), V((EL, W, D), F32), dma((3,)), dma((3, EL)), dma((5,)), dma((5,)),
            ],
            cost_estimate=pl.CostEstimate(flops=30_000_000_000, bytes_accessed=32_000_000, transcendentals=0),
            compiler_params=pltpu.CompilerParams(vmem_limit_bytes=60 * 1024 * 1024),
        )(nr, ur, act, gs, gsd, gr, y)
        z = lax.axis_index("etp")
        left = jnp.where(z == 0, dxh, jnp.where(z == 1, near, jnp.where(z == 2, far, across)))
        right = jnp.where(z == 3, dxh, jnp.where(z == 2, near, jnp.where(z == 1, far, across)))
        dx = jnp.concatenate([left, right], axis=1)
        return y, dx, gg, gu, gd, g_sg, g_su, g_sd, g_r.T

    return jax.shard_map(step, mesh=mesh, in_specs=in_specs, out_specs=out_specs, check_vma=False)
```

```python
import jax
import jax.numpy as jnp
from jax import lax
from jax.experimental import pallas as pl
from jax.experimental.pallas import tpu as pltpu
from jax.sharding import PartitionSpec as P


EPS = 1e-5
F32 = jnp.float32
BF16 = jnp.bfloat16
MESH = pl.DeviceIdType.MESH
TL = 128
NEP = 4
T = TL * NEP
D = 1536
HD = D // 2
E = 40
EL = 10
CAP = 16
W = 128
MR = 32
FB = 32 // MR
PE = MR // CAP
NP = EL // PE
O0 = 0
N0 = O0 + NP
NM = N0 + NP
PR = D // 8
NC = 4
CR = TL // NC


def dot(a, b):
    return jnp.dot(a, b, preferred_element_type=F32)


def dot_t(a, b):
    return lax.dot_general(a, b, (((1,), (1,)), ((), ())), preferred_element_type=F32)


def tdot(a, b):
    return lax.dot_general(a, b, (((0,), (0,)), ((), ())), preferred_element_type=F32)


def glu(a, b):
    return (a * jax.nn.sigmoid(a) * b).astype(BF16)


def glu_grads(dh, a, b):
    sig = jax.nn.sigmoid(a)
    d_gate = (dh * b * sig * (1.0 + a * (1.0 - sig))).astype(BF16)
    d_up = (dh * a * sig).astype(BF16)
    return d_gate, d_up


def line_kernel(
    x_h, dy_h, prim_v, alt_v, wr_v, wg_h, wu_h, wd_h, sg_h, su_h, sd_h,
    y_o, dx_o, nr_o, ur_o, act_o, gs_o, gsd_o, gr_o,
    x_a, dy_a, n_a, u_a, ids, wg, wu, wd, wsh, sd, s_v, ds_v, nr, ur, act, sact, dl, gs, gsd, gr,
    part, recv, o_all, dn_all, yb, dxb, dgb, pjb, qb, xrow, tgt_v, g_v, df_v, dnr_v, ab,
    xl, wl, sl, ids_s, ids_r, xs, xr, zs, zr, es, er, ys, yr, dgs, dgr, pjs, pjr, w1s, w1r, w2s, w2r, qs, qr, outs,
):
    z = lax.axis_index("etp")
    e = lax.axis_index("ep")
    dp = lax.axis_index("dp")
    e_y, e_c, e_d = e ^ 2, e ^ 1, e ^ 3
    peers = (e_y, e_c, e_d)
    is_end = (z == 0) | (z == 3)
    is_mid = (z == 1) | (z == 2)
    hs = z // 3

    def rows(j):
        return pl.ds(pl.multiple_of(j * TL, TL), TL)

    mine = rows(e)
    lx = pltpu.make_async_copy(x_h, x_a.at[mine], xl.at[0])
    ldy = pltpu.make_async_copy(dy_h, dy_a.at[mine], xl.at[1])
    lx.start()
    ldy.start()
    shared_loads = [pltpu.make_async_copy(a, b, sl.at[k]) for k, (a, b) in enumerate(((sg_h, wsh.at[z, 0]), (su_h, wsh.at[z, 1]), (sd_h, sd)))]
    for c in shared_loads:
        c.start()

    def wload(k, i):
        src, dst = ((wg_h, wg), (wu_h, wu), (wd_h, wd))[k]
        return pltpu.make_async_copy(src.at[i], dst.at[i], wl.at[k, i])

    ids[e] = jnp.zeros((8, TL), F32)
    ids[e, 0:1, :] = prim_v[...].astype(F32)
    ids[e, 1:2, :] = alt_v[...].astype(F32)

    barrier = pltpu.get_barrier_semaphore()
    for q in peers:
        pl.semaphore_signal(barrier, inc=1, device_id={"ep": q}, device_id_type=MESH)
    for k in range(1, 4):
        pl.semaphore_signal(barrier, inc=1, device_id={"etp": lax.rem(z + k, 4)}, device_id_type=MESH)
    pl.semaphore_signal(barrier, inc=1, device_id={"dp": 1 - dp}, device_id_type=MESH)
    for q in peers:
        pl.semaphore_signal(barrier, inc=1, device_id={"etp": 3 - z, "ep": q}, device_id_type=MESH)
    for c in shared_loads:
        c.wait()
    wsh[z, 2] = sd[...].T
    pl.semaphore_wait(barrier, 10)

    def rcopy(src, dst, s, r, dev):
        return pltpu.make_async_remote_copy(src_ref=src, dst_ref=dst, send_sem=s, recv_sem=r, device_id=dev, device_id_type=MESH)

    ids_c = [rcopy(ids.at[e], ids.at[e], ids_s.at[k], ids_r.at[k], {"ep": peers[k]}) for k in range(3)]
    for c in ids_c:
        c.start()
    lx.wait()
    x_c, relays = [], []
    for k, buf in enumerate((x_a, dy_a)):
        if k == 1:
            ldy.wait()
        pair = [
            rcopy(buf.at[mine], buf.at[mine], xs.at[k, 0], xr.at[k, 0], {"ep": e_y}),
            rcopy(buf.at[mine], buf.at[mine], xs.at[k, 1], xr.at[k, 1], {"ep": e_c}),
        ]
        for c in pair:
            c.start()
        x_c.append(pair)
        relays.append(rcopy(buf.at[rows(e_y)], buf.at[rows(e_y)], xs.at[k, 2], xr.at[k, 2], {"ep": e_c}))

    def load_body(i, _):
        for k in range(3):
            wload(k, i).start()
        return 0

    lax.fori_loop(0, EL, load_body, 0)

    def line_copy(d, m):
        return rcopy(part.at[d, m], recv.at[d, m], zs.at[d, m], zr.at[d, m], {"etp": jnp.clip(z - 1 + 2 * d, 0, 3)})

    def source_send(m):
        @pl.when(z == 3)
        def _():
            line_copy(0, m).start()

        @pl.when(z == 0)
        def _():
            line_copy(1, m).start()

    def take(d, m):
        line_copy(d, m).wait_recv()
        part[d, m] = part[d, m] + recv[d, m]

    def forward(hop, m):
        @pl.when(is_mid)
        def _():
            d = (2 - z) if hop == 1 else (z - 1)
            take(d, m)
            line_copy(d, m).start()

    def norm(xw):
        inv = lax.rsqrt(jnp.mean(xw * xw, axis=1, keepdims=True) + EPS)
        return inv, (xw * inv).astype(BF16)

    def shared_acts(n, dy, j):
        a = dot(n, wsh[j, 0])
        b = dot(n, wsh[j, 1])
        h = glu(a, b)
        dg_, du_ = glu_grads(dot(dy, wsh[j, 2]), a, b)
        return h, dg_, du_

    def piece(dp_, e_):
        return pl.ds(pl.multiple_of((dp_ * NEP + e_) * PR, 64), PR)

    def to_end(j, end):
        ref = wsh.at[j, :, piece(dp, e)]
        return rcopy(ref, ref, w1s.at[end // 3], w1r.at[j], {"etp": end})

    for end in (0, 3):
        @pl.when(z != end)
        def _(end=end):
            to_end(z, end).start()

    foreign = pl.ds(1 - hs, 3)

    def w_swap(k, dp_, e_, target, part_of=None):
        span = piece(dp_, e_)
        if part_of is not None:
            span = pl.ds(pl.multiple_of((dp_ * NEP + e_) * PR + part_of * (PR // 2), 32), PR // 2)
        ref = wsh.at[foreign, :, span]
        return rcopy(ref, ref, w2s.at[k], w2r.at[k], target)

    to_x, to_y, to_c = {"dp": 1 - dp}, {"ep": e_y}, {"ep": e_c}
    w_send = [
        w_swap(0, dp, e, to_x), w_swap(1, dp, e, to_y), w_swap(2, dp, e, to_c), w_swap(3, dp, e_y, to_x, 0),
        w_swap(4, 1 - dp, e, to_c), w_swap(5, dp, e_y, to_c), w_swap(6, 1 - dp, e_y, to_c), w_swap(7, 1 - dp, e, to_y, 1),
    ]
    w_recv = [
        w_swap(0, 1 - dp, e, to_x), w_swap(1, dp, e_y, to_y), w_swap(2, dp, e_c, to_c), w_swap(3, 1 - dp, e_y, to_x, 0),
        w_swap(4, 1 - dp, e_c, to_c), w_swap(5, dp, e_d, to_c), w_swap(6, 1 - dp, e_d, to_c), w_swap(7, 1 - dp, e_y, to_y, 1),
    ]

    for c in ids_c:
        c.wait_recv()
    cols = []
    for j in range(NEP):
        block = jnp.concatenate([ids[j], jnp.zeros((TL - 8, TL), F32)], axis=0)
        cols.append(jnp.transpose(block)[:, 0:2])
    idc = jnp.concatenate(cols, axis=0)
    prim, alt = idc[:, 0:1], idc[:, 1:2]
    iota_e = lax.broadcasted_iota(jnp.int32, (T, E), 1).astype(F32)
    one_p = jnp.where(prim == iota_e, 1.0, 0.0)
    earlier = jnp.where(
        lax.broadcasted_iota(jnp.int32, (T, T), 0) > lax.broadcasted_iota(jnp.int32, (T, T), 1), 1.0, 0.0
    ).astype(BF16)
    rank = jnp.sum(dot(earlier, one_p.astype(BF16)) * one_p, axis=1, keepdims=True)
    over = jnp.where(rank < CAP, 0.0, 1.0)
    kept = jnp.minimum(jnp.sum(one_p, axis=0, keepdims=True), float(CAP))
    one_a = jnp.where(alt == iota_e, 1.0, 0.0) * over
    slot_a = jnp.sum((dot(earlier, one_a.astype(BF16)) + kept) * one_a, axis=1, keepdims=True)
    keep_a = over * jnp.where(slot_a < CAP, 1.0, 0.0)
    one_s = one_p * (1.0 - over) + one_a * keep_a
    slot = (1.0 - over) * rank + keep_a * slot_a
    eid = jnp.sum(one_s * iota_e, axis=1, keepdims=True)
    has = (1.0 - over) + keep_a
    tgt_v[...] = jnp.where(has > 0.5, eid * CAP + slot, -1.0)
    df_v[...] = one_s

    base = (e * (EL * CAP)).astype(F32)
    pick = jnp.where(
        tgt_v[...] - base == lax.broadcasted_iota(jnp.int32, (T, EL * CAP), 1).astype(F32), 1.0, 0.0
    ).astype(BF16)

    def norm_rows(j):
        _, n = norm(x_a[rows(j), :].astype(F32))
        n_a[rows(j), :] = n

    norm_rows(e)
    x_c[0][1].wait_recv()
    norm_rows(e_c)
    x_c[0][0].wait_recv()
    relays[0].start()
    norm_rows(e_y)
    relays[0].wait_recv()
    norm_rows(e_d)
    nr[...] = tdot(pick, n_a[...]).astype(BF16)

    def expert_forward(k, _):
        for half in range(PE):
            i = PE * k + half
            for w in range(3):
                wload(w, i).wait()
            sl16 = pl.ds(pl.multiple_of(i * CAP, CAP), CAP)
            n_i = nr[sl16, :]
            a = dot(n_i, wg[i])
            b = dot(n_i, wu[i])
            h = glu(a, b)
            ab[0, sl16, :] = a
            ab[1, sl16, :] = b
            act[0, sl16, :] = h
            o = dot(h, wd[i])
            r16 = slice(half * CAP, (half + 1) * CAP)
            part[0, O0 + k, r16, :] = o[:, :HD]
            part[1, O0 + k, r16, :] = o[:, HD:]
        source_send(O0 + k)
        return 0

    lax.fori_loop(0, NP, expert_forward, 0)

    @pl.when(is_end)
    def _():
        for k in range(3):
            to_end(1 - hs + k, 0).wait_recv()
        for k in range(3):
            w_send[k].start()

    logits = dot_t(n_a[...], wr_v[...])
    ex = jnp.exp(logits - jnp.max(logits, axis=1, keepdims=True))
    probs = ex / jnp.sum(ex, axis=1, keepdims=True)
    g_v[...] = jnp.sum(probs * df_v[...], axis=1, keepdims=True)
    df_v[...] = df_v[...] - probs
    for m in range(2 * FB):
        forward(1, m)

    x_c[1][0].wait_recv()
    relays[1].start()
    x_c[1][1].wait_recv()
    relays[1].wait_recv()

    def u_body(j, _):
        u_a[rows(j), :] = (g_v[rows(j), :] * dy_a[rows(j), :].astype(F32)).astype(BF16)
        return 0

    lax.fori_loop(0, NEP, u_body, 0)
    ur[...] = tdot(pick, u_a[...]).astype(BF16)

    @pl.when(is_end)
    def _():
        xrow[...] = tdot(pick, x_a[...]).astype(BF16)


    def expert_backward(k, _):
        for half in range(PE):
            i = PE * k + half
            sl16 = pl.ds(pl.multiple_of(i * CAP, CAP), CAP)
            da, db = glu_grads(dot_t(ur[sl16, :], wd[i]), ab[0, sl16, :], ab[1, sl16, :])
            act[1, sl16, :] = da
            act[2, sl16, :] = db
            dn = dot_t(da, wg[i]) + dot_t(db, wu[i])
            r16 = slice(half * CAP, (half + 1) * CAP)
            part[0, N0 + k, r16, :] = dn[:, :HD]
            part[1, N0 + k, r16, :] = dn[:, HD:]
        source_send(N0 + k)
        forward(1, 2 * FB + k)
        forward(2, k)
        return 0

    lax.fori_loop(0, NP, expert_backward, 0)
    stores = [
        pltpu.make_async_copy(nr, nr_o, outs.at[2]),
        pltpu.make_async_copy(ur, ur_o, outs.at[3]),
        pltpu.make_async_copy(act, act_o, outs.at[4]),
    ]
    for c in stores:
        c.start()

    def sact_body(j):
        h, da, db = shared_acts(n_a[rows(j), :], dy_a[rows(j), :], z)
        sact[0, rows(j), :] = h
        sact[1, rows(j), :] = da
        sact[2, rows(j), :] = db
        return 0

    def shared_grads(c, _):
        cols = pl.ds(pl.multiple_of(c * W, W), W)
        n_c = n_a[:, cols]
        gs[0, cols, :] = tdot(n_c, sact[1])
        gs[1, cols, :] = tdot(n_c, sact[2])
        gsd[:, cols] = tdot(sact[0], dy_a[:, cols])
        return 0

    def piece_a(k):
        sact_body(2 * k)
        sact_body(2 * k + 1)

    def piece_b(k):
        lax.fori_loop(4 * k - 8, 4 * k - 4, shared_grads, 0)

    @pl.when(is_mid)
    def _():
        for k in range(NP):
            if k < NP - 2 * FB:
                forward(1, NP + 2 * FB + k)
            forward(2, NP + k)
            if k % FB == FB - 1:
                if k // FB < 2:
                    piece_a(k // FB)
                else:
                    piece_b(k // FB)

    def exchange(t, k, p):
        ref = (o_all, dn_all)[t].at[e_y if p == 2 else e, k]
        return rcopy(ref, ref, es.at[t, k, p], er.at[t, k, p], {"ep": e_y if p == 0 else e_c})

    def pass_on(t, k):
        exchange(t, k, 0).wait_recv()
        exchange(t, k, 2).start()

    lanes = pl.ds(pl.multiple_of(hs * HD, 128), HD)

    def place(n_rows, start):
        t_col = tgt_v[pl.ds(start, n_rows), :]
        return jnp.where(
            t_col == lax.broadcasted_iota(jnp.int32, (n_rows, E * CAP), 1).astype(F32), 1.0, 0.0
        ).astype(BF16)

    def col_to_row(col):
        return jnp.transpose(jnp.broadcast_to(col, (TL, TL)))[0:1, :]

    def dg_copy(h, k):
        return rcopy(dgb.at[h], dgb.at[h], dgs.at[k], dgr.at[h], {"etp": lax.rem(z + k + 1, 4)})

    def pj_copy():
        return rcopy(pjb.at[hs], pjb.at[hs], pjs.at[0], pjr.at[0], {"etp": 3 - z})

    def end_take_o(k, _):
        take(hs, O0 + k)
        o_all[e, k] = part[hs, O0 + k].astype(BF16)
        for p in range(2):
            exchange(0, k, p).start()

        @pl.when(k >= 2 * FB)
        def _():
            pass_on(0, k - 2 * FB)

        return 0

    def q_copy(r):
        ref = qb.at[hs, e]
        return rcopy(ref, ref, qs.at[r], qr.at[r], {"etp": 3 - z, "ep": e ^ r})

    def end_take_dn(k, _):
        take(hs, N0 + k)
        rounded = part[hs, N0 + k].astype(BF16)
        dn_all[e, k] = rounded
        for p in range(2):
            exchange(1, k, p).start()
        q = jnp.sum(rounded.astype(F32) * xrow[pl.ds(pl.multiple_of(k * MR, MR), MR), lanes].astype(F32), axis=1, keepdims=True)
        diag = lax.broadcasted_iota(jnp.int32, (MR, 128), 0) == lax.broadcasted_iota(jnp.int32, (MR, 128), 1)
        q_row = jnp.sum(jnp.where(diag, q, 0.0), axis=0, keepdims=True)
        at_k = lax.broadcasted_iota(jnp.int32, (16, 128), 0) == k
        qb[hs, e] = jnp.where(at_k, q_row, jnp.where(k == 0, 0.0, qb[hs, e]))

        @pl.when(k >= 2 * FB)
        def _():
            pass_on(1, k - 2 * FB)

        return 0

    def wait_exchange(t):
        for k in range(NP - 2 * FB, NP):
            pass_on(t, k)

        def body(k, _):
            exchange(t, k, 1).wait_recv()
            exchange(t, k, 2).wait_recv()
            return 0

        lax.fori_loop(0, NP, body, 0)

    def relay_copy(t, h, c):
        return rcopy(yb.at[t, h, c], yb.at[t, h, c], ys.at[t, h, c], yr.at[t, h, c], {"etp": jnp.clip(z + 1 - 2 * h, 0, 3)})

    def relay_start(t):
        for c in range(NC):
            relay_copy(t, hs, c).start()

    @pl.when(is_end)
    def _():
        w_recv[0].wait_recv()
        w_send[4].start()
        w_send[7].start()

        def takes(fn, g, n=1):
            lax.fori_loop(g * FB, (g + n) * FB, fn, 0)

        takes(end_take_o, 0)
        piece_a(0)
        w_recv[1].wait_recv()
        w_send[3].start()
        w_send[5].start()
        takes(end_take_o, 1)
        piece_a(1)
        takes(end_take_o, 2)
        w_recv[3].wait_recv()
        w_recv[7].wait_recv()
        w_send[6].start()
        takes(end_take_o, 3)
        piece_b(2)
        takes(end_take_o, 4)
        for k in (2, 4, 5, 6):
            w_recv[k].wait_recv()
        half = pl.ds(pl.multiple_of(hs * HD, 128), HD)

        def slice_body(j, _):
            h, da, db = shared_acts(n_a[mine, :], dy_a[mine, :], j)
            s_j = dot_t(h, wsh[j, 2, half, :])
            ds_j = dot_t(da, wsh[j, 0, half, :]) + dot_t(db, wsh[j, 1, half, :])
            s_v[...] += s_j
            ds_v[...] += ds_j
            return 0

        s_v[...] = jnp.zeros_like(s_v)
        ds_v[...] = jnp.zeros_like(ds_v)
        lax.fori_loop(0, 4, slice_body, 0)
        pjb[hs, 0:1, :] = col_to_row(jnp.sum(ds_v[...] * x_a[mine, lanes].astype(F32), axis=1, keepdims=True))
        pj_copy().start()
        takes(end_take_dn, 0)
        wait_exchange(0)
        o_flat = o_all[...].reshape(E * CAP, HD)
        tok = dot(place(TL, pl.multiple_of(e * TL, TL)), o_flat)
        y = (x_a[mine, lanes].astype(F32) + s_v[...] + g_v[mine, :] * tok).astype(BF16)
        for c in range(NC):
            yb[0, hs, c] = y[c * CR : (c + 1) * CR, :]
        relay_start(0)
        lane = lax.broadcasted_iota(jnp.int32, (TL, TL), 1)
        packed = jnp.zeros((TL, TL), F32)
        for j in range(NEP):
            tok = dot(place(TL, j * TL), o_flat)
            prod = dy_a[j * TL : (j + 1) * TL, lanes].astype(F32) * tok
            packed = jnp.where(lane == j, jnp.sum(prod, axis=1, keepdims=True), packed)
        dgb[hs] = jnp.transpose(packed)[0:8, :]
        for k in range(3):
            dg_copy(hs, k).start()
        takes(end_take_dn, 1)
        piece_b(3)
        takes(end_take_dn, 2)
        piece_b(4)
        takes(end_take_dn, 3, 2)
        for r in range(4):
            q_copy(r).start()

    late = [pltpu.make_async_copy(gs, gs_o, outs.at[0]), pltpu.make_async_copy(gsd, gsd_o, outs.at[1])]
    for c in late:
        c.start()
    stores += late

    def wait_dg():
        @pl.when(z != 0)
        def _():
            dg_copy(0, 0).wait_recv()

        @pl.when(z != 3)
        def _():
            dg_copy(1, 0).wait_recv()

    def make_dl():
        dg_rows = jnp.concatenate([dgb[0] + dgb[1], jnp.zeros((TL - 8, TL), F32)], axis=0)
        dg_cols = jnp.transpose(dg_rows)
        for j in range(NEP):
            sl_j = slice(j * TL, (j + 1) * TL)
            dl[sl_j, :] = (dg_cols[:, j : j + 1] * g_v[sl_j, :] * df_v[sl_j, :]).astype(BF16)

    def router_grad():
        gr[...] = tdot(dl[...], n_a[...])

    def relay_wait(t, h, c):
        relay_copy(t, h, c).wait_recv()

    def relay_through(t):
        def hop(n, c):
            h = (z - 1) if n == 1 else (2 - z)
            relay_wait(t, h, c)
            relay_copy(t, h, c).start()

        @pl.when(is_mid)
        def _():
            for c in range(NC + 2):
                if c < NC:
                    hop(1, c)
                if c >= 2:
                    hop(2, c - 2)

        @pl.when(is_end)
        def _():
            for c in range(NC):
                relay_wait(t, 1 - hs, c)

    @pl.when(is_mid)
    def _():
        relay_through(0)
        wait_dg()
        make_dl()
        router_grad()

    @pl.when(is_end)
    def _():
        wait_dg()
        make_dl()
        dn_r = dot(dl[mine, :], wr_v[...])
        dnr_v[0] = dn_r[:, :HD]
        dnr_v[1] = dn_r[:, HD:]
        router_grad()
        wait_exchange(1)
        tok = dot(place(TL, pl.multiple_of(e * TL, TL)), dn_all[...].reshape(E * CAP, HD))
        dn = ds_v[...] + dnr_v[hs] + tok
        other_lanes = pl.ds(pl.multiple_of((1 - hs) * HD, 128), HD)
        own = jnp.sum(dn * x_a[mine, lanes].astype(F32), axis=1, keepdims=True)
        rest = jnp.sum(dnr_v[1 - hs] * x_a[mine, other_lanes].astype(F32), axis=1, keepdims=True)
        inv, _ = norm(x_a[mine, :].astype(F32))
        pj_copy().wait_recv()
        far_s = jnp.transpose(jnp.broadcast_to(pjb[1 - hs, 0:1, :], (TL, TL)))[:, 0:1]
        dnr_v[hs] = dn
        for r in range(4):
            q_copy(r).wait_recv()
        t_own = tgt_v[mine, :]
        lane = lax.broadcasted_iota(jnp.int32, (TL, 128), 1).astype(F32)

        def q_body(i, acc):
            start = (i * MR).astype(F32)
            hit = (t_own - start == lane) & (lane < MR)
            return acc + jnp.where(hit, qb[1 - hs, i // NP, pl.ds(lax.rem(i, NP), 1), :], 0.0)

        picked = lax.fori_loop(0, NEP * NP, q_body, jnp.zeros((TL, 128), F32))
        proj = (own + rest + far_s + jnp.sum(picked, axis=1, keepdims=True)) * (1.0 / D)
        dx = (dy_a[mine, lanes].astype(F32) + inv * dnr_v[hs] - x_a[mine, lanes].astype(F32) * (inv * inv * inv) * proj).astype(BF16)
        dxb[...] = dx

    @pl.when(is_end)
    def _():
        relay_through(0)

    @pl.when(is_mid)
    def _():
        dxb[...] = jnp.zeros_like(dxb)

    st = pltpu.make_async_copy(gr, gr_o, outs.at[5])
    st.start()
    stores.append(st)

    def out_copies(t, out):
        cs = []
        for h in range(2):
            for c in range(NC):
                cs.append(pltpu.make_async_copy(yb.at[t, h, c], out.at[pl.ds(c * CR, CR), pl.ds(h * HD, HD)], outs.at[7 + t * 2 * NC + h * NC + c]))
        return cs

    oc = out_copies(0, y_o)
    for c in oc:
        c.start()
    stores += oc
    st = pltpu.make_async_copy(dxb, dx_o, outs.at[6])
    st.start()
    stores.append(st)

    for c in ids_c:
        c.wait_send()
    for k in range(2):
        for c in x_c[k]:
            c.wait_send()
        relays[k].wait_send()

    for end in (0, 3):
        @pl.when(z != end)
        def _(end=end):
            to_end(z, end).wait_send()

    @pl.when(is_end)
    def _():
        for c in w_send:
            c.wait_send()

    def line_drain(m, _):
        @pl.when(z != 0)
        def _():
            line_copy(0, m).wait_send()

        @pl.when(z != 3)
        def _():
            line_copy(1, m).wait_send()

        return 0

    lax.fori_loop(0, NM, line_drain, 0)

    @pl.when(is_end)
    def _():
        def drain(k, _):
            for t in range(2):
                for p in range(3):
                    exchange(t, k, p).wait_send()
            return 0

        lax.fori_loop(0, NP, drain, 0)
        for k in range(3):
            dg_copy(hs, k).wait_send()
        pj_copy().wait_send()
        for r in range(4):
            q_copy(r).wait_send()

    for t in range(1):
        for c in range(NC):
            @pl.when(z != 3)
            def _(t=t, c=c):
                relay_copy(t, 0, c).wait_send()

            @pl.when(z != 0)
            def _(t=t, c=c):
                relay_copy(t, 1, c).wait_send()

    for c in stores:
        c.wait()


def grads_kernel(nr_h, ur_h, act_h, gs_h, gsd_h, gr_h, y_h, gg_o, gu_o, gd_o, gsg_o, gsu_o, gsd_o, gr_o, y_o, nr, ur, act, gs, gsd, gr, yv, gg, gu, gd, ri, ro, li, so):
    first = [pltpu.make_async_copy(a, b, ri.at[k]) for k, (a, b) in enumerate(((nr_h, nr), (ur_h, ur), (act_h, act)))]
    through = ((gs_h.at[0], gs.at[0], gsg_o), (gs_h.at[1], gs.at[1], gsu_o), (gsd_h, gsd, gsd_o), (gr_h, gr, gr_o), (y_h, yv, y_o))
    loads = [pltpu.make_async_copy(a, b, li.at[k]) for k, (a, b, _) in enumerate(through)]
    stores = [pltpu.make_async_copy(b, c, so.at[k]) for k, (_, b, c) in enumerate(through)]
    for c in first:
        c.start()
    for c in loads:
        c.start()
    for c in first:
        c.wait()

    def out(k, i):
        src, dst = ((gg, gg_o), (gu, gu_o), (gd, gd_o))[k]
        return pltpu.make_async_copy(src.at[i], dst.at[i], ro.at[k, i])

    def body(i, _):
        r = pl.ds(pl.multiple_of(i * CAP, CAP), CAP)
        n = nr[r, :]
        gg[i] = tdot(n, act[1, r, :])
        out(0, i).start()
        gu[i] = tdot(n, act[2, r, :])
        out(1, i).start()
        gd[i] = tdot(act[0, r, :], ur[r, :])
        out(2, i).start()
        return 0

    lax.fori_loop(0, EL, body, 0)
    for a, b in zip(loads, stores):
        a.wait()
        b.start()
    for c in stores:
        c.wait()

    def drain(i, _):
        for k in range(3):
            out(k, i).wait()
        return 0

    lax.fori_loop(0, EL, drain, 0)


def solution(mesh):
    tok = P(("dp", "ep"), None)
    ids = P(("dp", "ep"))
    in_specs = (tok, tok, ids, ids, P(None, None), P("ep", None, "etp"), P("ep", None, "etp"), P("ep", "etp", None), P(None, "etp"), P(None, "etp"), P("etp", None))
    out_specs = (tok, tok, P(("dp", "ep"), None, "etp"), P(("dp", "ep"), None, "etp"), P(("dp", "ep"), "etp", None), P("dp", "etp"), P("dp", "etp"), P(("dp", "etp"), None), P("dp", None))
    any_ = pl.BlockSpec(memory_space=pl.ANY)
    vmem = pl.BlockSpec(memory_space=pltpu.VMEM)
    dma = pltpu.SemaphoreType.DMA

    def sds(shape, dtype):
        return jax.ShapeDtypeStruct(shape, dtype)

    def step(x, dy, prim, alt, wr, eg, eu, ed, sg, su, sd):
        outs = [
            sds((TL, D), BF16), sds((TL, HD), BF16), sds((EL * CAP, D), BF16), sds((EL * CAP, D), BF16), sds((3, EL * CAP, W), BF16),
            sds((2, D, W), F32), sds((W, D), F32), sds((E, D), F32),
        ]
        V = pltpu.VMEM
        scratch = [
            V((T, D), BF16), V((T, D), BF16), V((T, D), BF16), V((T, D), BF16), V((NEP, 8, TL), F32),
            V((EL, D, W), BF16), V((EL, D, W), BF16), V((EL, W, D), BF16), V((4, 3, D, W), BF16), V((W, D), BF16), V((TL, HD), F32), V((TL, HD), F32),
            V((EL * CAP, D), BF16), V((EL * CAP, D), BF16), V((3, EL * CAP, W), BF16), V((3, T, W), BF16), V((T, E), BF16), V((2, D, W), F32), V((W, D), F32), V((E, D), F32),
            V((2, NM, MR, HD), F32), V((2, NM, MR, HD), F32), V((NEP, NP, MR, HD), BF16), V((NEP, NP, MR, HD), BF16),
            V((1, 2, NC, CR, HD), BF16), V((TL, HD), BF16), V((2, 8, TL), F32), V((2, 8, TL), F32), V((2, NEP, 16, 128), F32), V((EL * CAP, D), BF16), V((T, 1), F32), V((T, 1), F32), V((T, E), F32), V((2, TL, HD), F32), V((2, EL * CAP, W), F32),
            dma((2,)), dma((3, EL)), dma((3,)), dma((3,)), dma((3,)), dma((2, 3)), dma((2, 3)), dma((2, NM)), dma((2, NM)),
            dma((2, NP, 3)), dma((2, NP, 3)), dma((1, 2, NC)), dma((1, 2, NC)), dma((3,)), dma((2,)), dma((1,)), dma((1,)), dma((2,)), dma((4,)), dma((8,)), dma((8,)), dma((4,)), dma((4,)), dma((7 + 4 * NC,)),
        ]
        y, dxh, nr, ur, act, gs, gsd, gr = pl.pallas_call(
            line_kernel,
            name="line",
            out_shape=outs,
            in_specs=[any_, any_, vmem, vmem, vmem] + [any_] * 6,
            out_specs=[any_] * 8,
            scratch_shapes=scratch,
            compiler_params=pltpu.CompilerParams(collective_id=0, has_side_effects=True, vmem_limit_bytes=60 * 1024 * 1024),
        )(x, dy, prim.reshape(1, TL), alt.reshape(1, TL), wr.T, eg, eu, ed, sg, su, sd)

        across = lax.ppermute(dxh, "etp", [(0, 3), (3, 0)])
        far = lax.ppermute(dxh, "etp", [(0, 2), (3, 1)])
        near = lax.ppermute(dxh, "etp", [(0, 1), (3, 2)])
        gg, gu, gd, g_sg, g_su, g_sd, g_r, y = pl.pallas_call(
            grads_kernel,
            name="grads",
            out_shape=[
                sds((EL, D, W), F32), sds((EL, D, W), F32), sds((EL, W, D), F32),
                sds((D, W), F32), sds((D, W), F32), sds((W, D), F32), sds((E, D), F32), sds((TL, D), BF16),
            ],
            in_specs=[any_] * 7,
            out_specs=[any_] * 8,
            scratch_shapes=[
                V((EL * CAP, D), BF16), V((EL * CAP, D), BF16), V((3, EL * CAP, W), BF16), V((2, D, W), F32), V((W, D), F32), V((E, D), F32), V((TL, D), BF16),
                V((EL, D, W), F32), V((EL, D, W), F32), V((EL, W, D), F32), dma((3,)), dma((3, EL)), dma((5,)), dma((5,)),
            ],
            cost_estimate=pl.CostEstimate(flops=30_000_000_000, bytes_accessed=32_000_000, transcendentals=0),
            compiler_params=pltpu.CompilerParams(vmem_limit_bytes=60 * 1024 * 1024),
        )(nr, ur, act, gs, gsd, gr, y)
        z = lax.axis_index("etp")
        left = jnp.where(z == 0, dxh, jnp.where(z == 1, near, jnp.where(z == 2, far, across)))
        right = jnp.where(z == 3, dxh, jnp.where(z == 2, near, jnp.where(z == 1, far, across)))
        dx = jnp.concatenate([left, right], axis=1)
        return y, dx, gg, gu, gd, g_sg, g_su, g_sd, g_r.T

    return jax.shard_map(step, mesh=mesh, in_specs=in_specs, out_specs=out_specs, check_vma=False)
```
